32 devices in a mesh: angle: 4 (over z), pos: 8 (over y, x, core).
Axes of the slice: x: 2, y: 2, z: 4, core: 2. Of those that a mesh axis runs over, the one named last changes fastest.
Arguments:
- amplitude: float32 [4, 32, 128, 128], P('angle', 'pos'), may hold values from 0 to 2.5
- offsets: int32 [4, 32, 2], P('angle', 'pos'), may hold values from 0 to 896, as said below
- probe_field: float32 [2, 128, 128], replicated, may hold values from -5 to 5
- object_field: float32 [4, 2, 1024, 1024], P('angle', None, 'pos'), may hold values from -5 to 5
- interp_index: int32 [4, 2, 1024], replicated, may hold values from 0 to 1022
- interp_weight: float32 [4, 2, 1024], replicated, may hold values from 0 to 1
Outputs:
- new_object: float32 [4, 2, 1024, 1024], P('angle', None, 'pos')
- new_probe: float32 [2, 128, 128], replicated
- recon: float32 [8, 128, 2, 1024], P('pos', 'angle')
The draws below stay inside these ranges and needn't reach their ends.
Inputs may be any that keep to these rules, and one draw needn't show every extreme that they name: For position j, offsets[a, j, 0] = max(0, min(896, (j // 4) * 128 - 128 // 2 + u)) with 0 <= u < 128; offsets[a, j, 1] lies in 0 to 896.
All inputs are finite; a program needn't handle non-finite values.
Results may differ from the reference program's by a relative error of at most 0.00007.
Values sent between devices are 32-bit elements; how exact they have to be, the bound alone decides.
A program may use at most 64 MiB of HBM per device.

```python
import math
import jax
import jax.numpy as jnp
from jax import lax

NOBJ = 1024
PATCH = 128
POS_DEV = 4
ZWIN = 2
ANGLES = 4
POSITIONS = 32
BAND = 128
N_POS = 8


def draw_offsets(key, part):
    key_rows = jax.random.fold_in(key, 11)
    key_cols = jax.random.fold_in(key, 12)
    owners = jnp.arange(POSITIONS, dtype=jnp.int32) // POS_DEV
    base = owners * BAND - PATCH // 2
    shifts = jax.random.randint(key_rows, (ANGLES, POSITIONS), 0, BAND, dtype=jnp.int32)
    first_rows = jnp.clip(base[None, :] + shifts, 0, NOBJ - PATCH)
    first_cols = jax.random.randint(key_cols, (ANGLES, POSITIONS), 0, NOBJ - PATCH + 1, dtype=jnp.int32)
    return jnp.stack([first_rows, first_cols], axis=-1).astype(jnp.int32)


def with_ends(array, own_key, low, high):
    longest = array.shape.index(max(array.shape))
    spots = []
    for shift in (0, 1):
        where = [jax.random.randint(jax.random.fold_in(own_key, axis), (), 0, length) for axis, length in enumerate(array.shape)]
        where[longest] = (where[longest] + shift) % array.shape[longest]
        spots.append(tuple(where))
    return array.at[spots[0]].set(low).at[spots[1]].set(high)


def block_scale(rng, dims, pieces, smallest, largest):
    factor_of, own = 1.0, jax.random.fold_in(rng, 6)
    for position, blocks in pieces:
        steps = jnp.exp(jax.random.uniform(jax.random.fold_in(own, position), (blocks,), jnp.float32, smallest / len(pieces), largest / len(pieces)))
        factor_of = factor_of * jnp.repeat(steps, dims[position] // blocks).reshape([-1 if axis == position else 1 for axis in range(len(dims))])
    return factor_of


def bell_draw(key, extent, scale, bound, split=(), kind=jnp.bfloat16):
    values = jax.random.normal(key, extent, jnp.float32) * scale
    if len(split) > 0:
        values = block_scale(key, extent, split, -0.22, 0.18) * values
    return jnp.clip(values, min=-bound, max=bound).astype(kind)


def setup_inputs(seed: int = 0) -> dict:
    seeds = jax.random.split(jax.random.key(seed), 7)
    amplitude = jnp.clip(2.5 * jax.random.uniform(seeds[0], (ANGLES, POSITIONS, PATCH, PATCH), jnp.float32) ** block_scale(seeds[0], (ANGLES, POSITIONS, PATCH, PATCH), ((0, 4), (1, 8)), -0.2, 0.2), 0.0, 2.5)
    offsets = draw_offsets(jax.random.fold_in(seeds[6], 71), 0)
    probe_field = bell_draw(seeds[2], (2, PATCH, PATCH), 0.8, 5.0, (), jnp.float32)
    object_field = bell_draw(seeds[3], (ANGLES, 2, NOBJ, NOBJ), 0.8, 5.0, ((0, 4), (2, 8)), jnp.float32)
    interp_index = with_ends(jax.random.randint(seeds[4], (ANGLES, ZWIN, NOBJ), 0, NOBJ - 1), jax.random.fold_in(seeds[4], 1), 0, (NOBJ - 1) - 1).astype(jnp.int32)
    interp_weight = jnp.clip(jax.random.uniform(seeds[5], (ANGLES, ZWIN, NOBJ), jnp.float32, 0.0, 1.0), 0.0, 1.0)
    return dict(amplitude=amplitude, offsets=offsets, probe_field=probe_field, object_field=object_field, interp_index=interp_index, interp_weight=interp_weight)


def ramp_matrix(length):
    ramp = jnp.arange(length, dtype=jnp.int32)
    differ = ramp[:, None] - ramp[None, :]
    spread = differ.astype(jnp.float32)
    squared = jnp.maximum(spread * spread, 1.0)
    odd_terms = jnp.where(differ % 2 != 0, -1.0 / (math.pi * math.pi * squared), 0.0)
    return jnp.where(differ == 0, 0.25, odd_terms).astype(jnp.float32)


def reference(amplitude, offsets, probe_field, object_field, interp_index, interp_weight):
    probe_c = lax.complex(probe_field[0], probe_field[1])
    power = probe_field[0] * probe_field[0] + probe_field[1] * probe_field[1]

    def one_angle(inputs):
        amps, places, layer = inputs
        field = lax.complex(layer[0], layer[1])

        def take_patch(place):
            return lax.dynamic_slice(field, (place[0], place[1]), (PATCH, PATCH))

        patches = jax.vmap(take_patch)(places)
        exit_wave = probe_c * patches
        spectrum = jnp.fft.fft2(exit_wave, norm="ortho")
        magnitude = jnp.abs(spectrum)
        fixed = spectrum * (amps / jnp.maximum(magnitude, 0.5))
        change = jnp.fft.ifft2(fixed, norm="ortho") - exit_wave
        contrib = jnp.conj(probe_c) * change
        numer = jnp.sum(jnp.conj(patches) * change, axis=0)
        denom = jnp.sum(jnp.real(patches) ** 2 + jnp.imag(patches) ** 2, axis=0)
        stacked = jnp.stack([jnp.real(contrib), jnp.imag(contrib), jnp.broadcast_to(power, contrib.shape)], axis=1)

        def accumulate(count, total):
            start = (jnp.int32(0), places[count, 0], places[count, 1])
            current = lax.dynamic_slice(total, start, (3, PATCH, PATCH))
            return lax.dynamic_update_slice(total, current + stacked[count], start)

        total = lax.fori_loop(0, POSITIONS, accumulate, jnp.zeros((3, NOBJ, NOBJ), jnp.float32))
        updated = layer + total[:2] / (total[2] + 1.0)
        return updated, jnp.stack([jnp.real(numer), jnp.imag(numer)]), denom

    new_object, numers, denoms = lax.map(one_angle, (amplitude, offsets, object_field))
    new_probe = probe_field + jnp.sum(numers, axis=0) / (jnp.sum(denoms, axis=0) + 1.0)
    sinogram = jnp.transpose(new_object[:, 1], (1, 0, 2))
    filtered = jnp.dot(sinogram.reshape(NOBJ * ANGLES, NOBJ), ramp_matrix(NOBJ), precision=lax.Precision.HIGHEST)
    filtered = jnp.moveaxis(filtered.reshape(NOBJ, ANGLES, NOBJ), 1, 0)

    def project_back(total, inputs):
        rows_angle, index_angle, weight_angle = inputs
        lower = jnp.take(rows_angle, index_angle, axis=1)
        upper = jnp.take(rows_angle, index_angle + 1, axis=1)
        return total + (1.0 - weight_angle) * lower + weight_angle * upper, None

    total, unused = lax.scan(project_back, jnp.zeros((NOBJ, ZWIN * NOBJ), jnp.float32),
                             (filtered, interp_index.reshape(ANGLES, ZWIN * NOBJ), interp_weight.reshape(ANGLES, ZWIN * NOBJ)))
    recon = (total * (math.pi / ANGLES)).reshape(N_POS, NOBJ // N_POS, ZWIN, NOBJ)
    return new_object, new_probe, recon
```

```python
import functools
import math

import jax
import jax.numpy as jnp
import numpy as np
from jax import lax
from jax.experimental import pallas as pl
from jax.experimental.pallas import tpu as pltpu
from jax.sharding import PartitionSpec as P

MESH = pl.DeviceIdType.MESH
VMEM = pltpu.VMEM
LANES = 128


def split_const(table):
    high = jnp.asarray(table, jnp.float32).astype(jnp.bfloat16)
    low = (jnp.asarray(table, jnp.float32) - high.astype(jnp.float32)).astype(jnp.bfloat16)
    return high, low


def dft_blocks(length):
    ramp = np.arange(length)
    theta = (ramp[:, None] * ramp[None, :] % length) * (2.0 * math.pi / length)
    real = np.cos(theta) / math.sqrt(length)
    imag = -np.sin(theta) / math.sqrt(length)
    left = np.block([[real, -imag], [imag, real]])
    right = np.block([[real, imag], [-imag, real]])
    return np.asarray(left, np.float32), np.asarray(right, np.float32)


def halves(value):
    high = value.astype(jnp.bfloat16)
    return high, (value - high.astype(jnp.float32)).astype(jnp.bfloat16)


def mm(a, b):
    return jnp.dot(a, b, preferred_element_type=jnp.float32)


def left3(table_high, table_low, value):
    high, low = halves(value)
    return mm(table_high, high) + mm(table_high, low) + mm(table_low, high)


def right3(value, table_high, table_low):
    high, low = halves(value)
    return mm(high, table_high) + mm(low, table_high) + mm(high, table_low)


def remote(src, dst, send, recv, axis, target):
    return pltpu.make_async_remote_copy(
        src_ref=src, dst_ref=dst, send_sem=send, recv_sem=recv,
        device_id={axis: target}, device_id_type=MESH,
    )


def flip(me, mask, bits):
    other = 0
    for b in range(bits):
        bit = (me // (1 << b)) % 2
        other = other + (1 << b) * (1 - bit if (mask >> b) & 1 else bit)
    return other


def step_kernel(n_ang, n_pos, size,
                offs_h, obj_h, amp_h, probe_h, index_h, weight_h, ah_h, al_h, bh_h, bl_h,
                newobj, recon, change,
                offs, near, offs_v, near_v, obj, amp, probe, index, weight, ah, al, bh, bl,
                ext, sb, zo, za, zb, accw, acci, accr, grad, from_above, from_below,
                numden, rs, partial, ag, piece, sino, tables, rh, rl,
                in_sem, near_sem, send_sem, recv_sem, rs_send, rs_recv,
                a2a_send, a2a_recv, ag_send, ag_recv, fin_send, fin_recv):
    me_a = lax.axis_index("angle")
    me = lax.axis_index("pos")
    up, down = lax.rem(me + n_pos - 1, n_pos), lax.rem(me + 1, n_pos)
    tiles, band = obj.shape[1], obj.shape[2]
    width = tiles * LANES
    patch = probe.shape[1]
    half = patch // 2
    count = amp.shape[1]
    ns = sino.shape[1]

    sources = [(offs_h, offs), (offs_h, offs_v), (probe_h, probe), (amp_h, amp),
               (ah_h, ah), (al_h, al), (bh_h, bh), (bl_h, bl), (index_h, index), (weight_h, weight)]
    sources += [(obj_h.at[0, :, :, pl.ds(t * LANES, LANES)], obj.at[:, t]) for t in range(tiles)]
    loads = [pltpu.make_async_copy(src, dst, in_sem.at[k]) for k, (src, dst) in enumerate(sources)]
    for copy in loads:
        copy.start()
    bits = (n_ang - 1).bit_length()
    order = [1] + list(range(n_ang - 1, 1, -1))
    angle_peers = [flip(me_a, mask, bits) for mask in order]
    pos_peers = [lax.rem(me + d, n_pos) for d in range(1, n_pos)]
    barrier = pltpu.get_barrier_semaphore()
    for peer in pos_peers:
        pl.semaphore_signal(barrier, inc=1, device_id={"pos": peer}, device_id_type=MESH)
    for peer in angle_peers:
        pl.semaphore_signal(barrier, inc=1, device_id={"angle": peer}, device_id_type=MESH)
    loads[1].wait()
    pl.semaphore_wait(barrier, n_ang + n_pos - 2)
    swap = [remote(offs_v, near_v.at[0], send_sem.at[0], recv_sem.at[0], "pos", down),
            remote(offs_v, near_v.at[1], send_sem.at[1], recv_sem.at[1], "pos", up)]
    for copy in swap:
        copy.start()
    loads[0].wait()
    for copy in loads[10:]:
        copy.wait()

    def columns(c, rows, col):
        tile = col // LANES
        after = jnp.minimum(tile + 1, tiles - 1)
        got = jnp.concatenate([obj[c, tile, rows, :], obj[c, after, rows, :]], axis=1)
        return pltpu.roll(got, lax.rem(2 * LANES - lax.rem(col, LANES), 2 * LANES), 1)[:, :patch]

    for j in range(count):
        for c in range(2):
            ext[j // size][j % size, c, half:half + band, :] = columns(c, slice(0, band), offs[1, j])
    zo[...] = jnp.zeros_like(zo)
    za[...] = jnp.zeros_like(za)
    zb[...] = jnp.zeros_like(zb)
    for k, copy in enumerate(swap):
        copy.wait()
    for k in range(2):
        pltpu.make_async_copy(near_v.at[k], near.at[k], near_sem.at[k]).start()
    for k in range(2):
        pltpu.make_async_copy(near_v.at[k], near.at[k], near_sem.at[k]).wait()
    first = []
    groups = [range(g * size, (g + 1) * size) for g in range(count // size)]
    for g, group in enumerate(groups):
        for j in group:
            for c in range(2):
                sb[0, j, c] = columns(c, slice(band - half, band), near[1, 1, j])
                sb[1, j, c] = columns(c, slice(0, half), near[0, 1, j])
        span = pl.ds(g * size, size)
        pair = [
            remote(sb.at[0, span], ext[g].at[:, :, pl.ds(0, half), :],
                   send_sem.at[2 + 4 * g], recv_sem.at[2 + 4 * g], "pos", down),
            remote(sb.at[1, span], ext[g].at[:, :, pl.ds(half + band, half), :],
                   send_sem.at[3 + 4 * g], recv_sem.at[3 + 4 * g], "pos", up),
        ]
        for copy in pair:
            copy.start()
        first.append(pair)

    def spot(row, col, owner):
        return jnp.clip(row - owner * band + half, 0, band), col

    own_at = [spot(offs[0, j], offs[1, j], me) for j in range(count)]
    above_at = [spot(near[0, 0, j], near[0, 1, j], up) for j in range(count)]
    below_at = [spot(near[1, 0, j], near[1, 1, j], down) for j in range(count)]

    def wide(plane, col):
        blank = jnp.zeros((plane.shape[0], LANES), jnp.float32)
        both = jnp.concatenate([plane, blank], axis=1)
        return pltpu.roll(both, lax.rem(col, LANES), 1)

    lead = max(0, band - half)

    def place(acc, buf, first_row, plane, start, rows, col):
        shifted = wide(plane, col)
        where = slice(first_row, first_row + plane.shape[0])
        buf[tiles - 1, where, :] = shifted[:, :LANES]
        buf[tiles, where, :] = shifted[:, LANES:]
        begin = tiles - 1 - col // LANES
        for t in range(tiles):
            acc[t, rows, :] = acc[t, rows, :] + buf[begin + t, pl.ds(start, rows.stop - rows.start), :]

    def place_own(acc, plane, j):
        row, col = own_at[j]
        place(acc, zo, lead, plane, lead + half - row, slice(0, band), col)

    def place_above(acc, plane, j):
        row, col = above_at[j]
        place(acc, za, 0, plane, band - row, slice(0, half), col)

    def place_below(acc, plane, j):
        row, col = below_at[j]
        place(acc, zb, band, plane, band - row, slice(band - half, band), col)

    loads[2].wait()
    p_re, p_im = probe[0], probe[1]
    power = p_re * p_re + p_im * p_im
    accw[...] = jnp.ones_like(accw)
    acci[...] = jnp.zeros_like(acci)
    accr[...] = jnp.zeros_like(accr)
    for j in range(count):
        place_own(accw, power, j)
        place_above(accw, power[half:], j)
        place_below(accw, power[:half], j)
    accw[...] = 1.0 / accw[...]
    tall = 64

    def ramp(step, carry):
        top = pl.multiple_of(step * tall, tall)
        shape = (tall, width)
        differ = lax.broadcasted_iota(jnp.int32, shape, 1) - (
            lax.broadcasted_iota(jnp.int32, shape, 0) + top)
        spread = differ.astype(jnp.float32)
        odd = -1.0 / (jnp.maximum(spread * spread, 1.0) * (math.pi * math.pi))
        value = jnp.where((differ & 1) == 1, odd, jnp.where(differ == 0, 0.25, 0.0))
        rh[pl.ds(top, tall), :], rl[pl.ds(top, tall), :] = halves(value)
        return carry

    lax.fori_loop(0, width // tall, ramp, 0)
    for copy in loads[3:10]:
        copy.wait()
    n_re = jnp.zeros((patch, patch), jnp.float32)
    n_im = n_re
    den = n_re
    second = []
    for g, group in enumerate(groups):
        for copy in first[g]:
            copy.wait()
        q_re, q_im, w_re, w_im = [], [], [], []
        for j in group:
            rows = pl.ds(own_at[j][0], patch)
            re, im = ext[g][j % size, 0, rows, :], ext[g][j % size, 1, rows, :]
            q_re.append(re)
            q_im.append(im)
            w_re.append(p_re * re - p_im * im)
            w_im.append(p_re * im + p_im * re)
        psi = jnp.concatenate([jnp.concatenate(w_re, axis=1), jnp.concatenate(w_im, axis=1)], axis=0)
        mid = left3(ah[...], al[...], psi)
        cells = [slice(n * patch, (n + 1) * patch) for n in range(size)]
        rows = [jnp.concatenate([mid[:patch, cell], mid[patch:, cell]], axis=1) for cell in cells]
        spec = right3(jnp.concatenate(rows, axis=0), bh[...], bl[...])
        fixed = []
        for j, cell in zip(group, cells):
            s_re = spec[cell, :patch]
            s_im = spec[cell, patch:]
            factor = amp[0, j] / jnp.maximum(jnp.sqrt(s_re * s_re + s_im * s_im), 0.5)
            fixed.append(jnp.concatenate([factor * s_re, factor * s_im], axis=1))
        back = right3(jnp.concatenate(fixed, axis=0), ah[...], al[...])
        wide_re = jnp.concatenate([back[cell, :patch] for cell in cells], axis=1)
        wide_im = jnp.concatenate([back[cell, patch:] for cell in cells], axis=1)
        diff = left3(bh[...], bl[...], jnp.concatenate([wide_re, wide_im], axis=0))
        diff = diff - psi
        for n, j in enumerate(group):
            d_re, d_im = diff[:patch, cells[n]], diff[patch:, cells[n]]
            g_re = p_re * d_re + p_im * d_im
            g_im = p_re * d_im - p_im * d_re
            for h in range(2):
                grad[h, j, 0] = g_re[h * half:(h + 1) * half]
                grad[h, j, 1] = g_im[h * half:(h + 1) * half]
            n_re = n_re + (q_re[n] * d_re + q_im[n] * d_im)
            n_im = n_im + (q_re[n] * d_im - q_im[n] * d_re)
            den = den + (q_re[n] * q_re[n] + q_im[n] * q_im[n])
        span = pl.ds(g * size, size)
        pair = [
            remote(grad.at[1, span], from_above.at[span], send_sem.at[4 + 4 * g],
                   recv_sem.at[4 + 4 * g], "pos", down),
            remote(grad.at[0, span], from_below.at[span], send_sem.at[5 + 4 * g],
                   recv_sem.at[5 + 4 * g], "pos", up),
        ]
        for copy in pair:
            copy.start()
        second.append(pair)
    numden[0] = n_re
    numden[1] = n_im
    numden[2] = den
    pr = patch // n_pos
    scatter = [
        remote(numden.at[:, pl.ds(pl.multiple_of(peer * pr, 8), pr), :], rs.at[d],
               rs_send.at[d], rs_recv.at[d], "pos", peer)
        for d, peer in enumerate(pos_peers)
    ]
    for copy in scatter:
        copy.start()

    def whole_patch(j, c):
        return jnp.concatenate([grad[0, j, c], grad[1, j, c]], axis=0)

    for j in range(count):
        place_own(acci, whole_patch(j, 1), j)
    for g, group in enumerate(groups):
        for copy in second[g]:
            copy.wait()
        for j in group:
            place_above(acci, from_above[j, 1], j)
            place_below(acci, from_below[j, 1], j)
    for t in range(tiles):
        lanes = slice(t * LANES, (t + 1) * LANES)
        newobj[0, 1, :, lanes] = obj[1, t] + acci[t] * accw[t]
    across = [
        remote(newobj.at[0, 1, pl.ds(pl.multiple_of(peer * ns, 8), ns), :], sino.at[k],
               a2a_send.at[k], a2a_recv.at[k], "angle", peer)
        for k, peer in enumerate(angle_peers)
    ]
    for copy in across:
        copy.start()
    for j in range(count):
        place_own(accr, whole_patch(j, 0), j)
        place_above(accr, from_above[j, 0], j)
        place_below(accr, from_below[j, 0], j)
    for t in range(tiles):
        lanes = slice(t * LANES, (t + 1) * LANES)
        newobj[0, 0, :, lanes] = obj[0, t] + accr[t] * accw[t]
    for copy in scatter:
        copy.wait()
    part = numden[:, pl.ds(pl.multiple_of(me * pr, 8), pr), :]
    for d in range(n_pos - 1):
        part = part + rs[d]
    partial[...] = part
    gather = [
        remote(partial, ag.at[me_a], ag_send.at[k], ag_recv.at[k], "angle", peer)
        for k, peer in enumerate(angle_peers)
    ]
    for copy in gather:
        copy.start()

    chunk = tables.shape[2]
    per_row = width // chunk
    zwin = index.shape[1]
    per_angle = zwin * per_row
    bins = lax.broadcasted_iota(jnp.int32, (width, chunk), 0)

    def build(step, carry):
        a = step // per_angle
        z = lax.rem(step // per_row, zwin)
        lanes = pl.ds(pl.multiple_of(lax.rem(step, per_row) * chunk, chunk), chunk)
        hit = bins == index[a, pl.ds(z, 1), lanes]
        tables[step] = jnp.where(hit, 1.0, 0.0).astype(jnp.bfloat16)
        return carry

    lax.fori_loop(0, tables.shape[0], build, 0)

    def project(k, a, lines):
        high, low = halves(lines)
        both = mm(jnp.concatenate([high, low], axis=0), rh[...])
        lines = (both[:ns] + both[ns:] + mm(high, rl[...])) * (math.pi / n_ang)
        high, low = halves(lines)
        next_high, next_low = halves(pltpu.roll(lines, width - 1, 1))
        stack = jnp.concatenate([high, low, next_high, next_low], axis=0)
        for n in range(per_angle):
            z, part = n // per_row, n % per_row
            got = mm(stack, tables[a * per_angle + n])
            lower = got[:ns] + got[ns:2 * ns]
            upper = got[2 * ns:3 * ns] + got[3 * ns:]
            w = weight[pl.ds(a, 1), z, pl.ds(part * chunk, chunk)]
            value = (1.0 - w) * lower + w * upper
            lanes = pl.ds(n * chunk, chunk)
            recon[:, lanes] = value if k == 0 else recon[:, lanes] + value

    project(0, me_a, newobj[0, 1, pl.ds(pl.multiple_of(me_a * ns, 8), ns), :])
    ag[me_a] = partial[...]
    for copy in gather:
        copy.wait()
    total = ag[0]
    for a in range(1, n_ang):
        total = total + ag[a]
    mine = pl.ds(pl.multiple_of(me * pr, 8), pr)
    for c in range(2):
        value = total[c] / (total[2] + 1.0)
        piece[c] = value
        change[c, mine, :] = value
    spread = [
        remote(piece, change.at[:, mine, :], fin_send.at[d], fin_recv.at[d], "pos", peer)
        for d, peer in enumerate(pos_peers)
    ]
    for copy in spread:
        copy.start()
    for k, peer in enumerate(angle_peers):
        across[k].wait()
        project(k + 1, peer, sino[k])
    for copy in spread:
        copy.wait()


def tail_kernel(newobj, recon, change, probe, out_obj, out_probe, out_recon, sem):
    copy = pltpu.make_async_copy(newobj, out_obj, sem.at[0])
    copy.start()
    out_probe[...] = probe[...] + change[...]
    width = out_recon.shape[3]
    for s in range(out_recon.shape[1]):
        for z in range(out_recon.shape[2]):
            out_recon[0, s, z:z + 1, :] = recon[s:s + 1, z * width:(z + 1) * width]
    copy.wait()


def on_device(n_ang, n_pos, amplitude, offsets, probe_field, object_field, interp_index, interp_weight):
    band = object_field.shape[2]
    width = object_field.shape[3]
    patch = probe_field.shape[1]
    half = patch // 2
    count = offsets.shape[1]
    tiles = width // LANES
    f32, i32, bf16 = jnp.float32, jnp.int32, jnp.bfloat16
    n_z = interp_index.shape[1]
    chunk = min(512, width)
    tables = n_ang * n_z * (width // chunk)
    size = 2 if count % 2 == 0 else count
    left, right = dft_blocks(patch)
    ah, al = split_const(left)
    bh, bl = split_const(right)
    vmem = pl.BlockSpec(memory_space=VMEM)
    hbm = pl.BlockSpec(memory_space=pl.ANY)
    sds = jax.ShapeDtypeStruct
    dma = pltpu.SemaphoreType.DMA
    total = n_z * width
    ns = band // n_ang
    pr = patch // n_pos
    lead = max(0, band - half)
    ext = 2 * tiles
    table = VMEM((2 * patch, 2 * patch), bf16)
    half_shape = (count, 2, half, patch)
    links = 2 + 4 * (count // size)
    newobj, recon, change = pl.pallas_call(
        functools.partial(step_kernel, n_ang, n_pos, size),
        out_shape=(sds(object_field.shape, f32), sds((ns, total), f32), sds(probe_field.shape, f32)),
        in_specs=[hbm] * 10,
        out_specs=(vmem,) * 3,
        scratch_shapes=[
            pltpu.SMEM((2, count), i32), pltpu.SMEM((2, 2, count), i32),
            VMEM((2, count), i32), VMEM((2, 2, count), i32),
            VMEM((2, tiles, band, LANES), f32), VMEM(amplitude.shape, f32), VMEM(probe_field.shape, f32),
            VMEM(interp_index.shape, i32), VMEM(interp_weight.shape, f32),
            table, table, table, table,
            [VMEM((size, 2, band + patch, patch), f32)] * (count // size), VMEM((2,) + half_shape, f32),
            VMEM((ext, lead + half + band, LANES), f32),
            VMEM((ext, half + band, LANES), f32), VMEM((ext, half + band, LANES), f32),
            VMEM((tiles, band, LANES), f32), VMEM((tiles, band, LANES), f32), VMEM((tiles, band, LANES), f32),
            VMEM((2,) + half_shape, f32), VMEM(half_shape, f32), VMEM(half_shape, f32),
            VMEM((3, patch, patch), f32), VMEM((n_pos - 1, 3, pr, patch), f32),
            VMEM((3, pr, patch), f32), VMEM((n_ang, 3, pr, patch), f32), VMEM((2, pr, patch), f32),
            VMEM((n_ang - 1, ns, width), f32),
            VMEM((tables, width, chunk), bf16), VMEM((width, width), bf16), VMEM((width, width), bf16),
            dma((10 + tiles,)), dma((2,)), dma((links,)), dma((links,)), dma((n_pos - 1,)), dma((n_pos - 1,)),
            dma((n_ang - 1,)), dma((n_ang - 1,)), dma((n_ang - 1,)), dma((n_ang - 1,)),
            dma((n_pos - 1,)), dma((n_pos - 1,)),
        ],
        compiler_params=pltpu.CompilerParams(
            collective_id=0, has_side_effects=True, vmem_limit_bytes=KLIMIT),
        name="step",
    )(jnp.transpose(offsets[0]), object_field, amplitude, probe_field, interp_index, interp_weight, ah, al, bh, bl)
    out = pl.pallas_call(
        tail_kernel,
        out_shape=(sds(object_field.shape, f32), sds(probe_field.shape, f32), sds((1, ns, n_z, width), f32)),
        in_specs=[vmem] * 4,
        out_specs=(hbm, vmem, vmem),
        scratch_shapes=[dma((1,))],
        compiler_params=pltpu.CompilerParams(vmem_limit_bytes=TLIMIT),
        name="tail",
    )(newobj, recon, change, probe_field)
    return tuple(out)


KLIMIT = 56 * 1024 * 1024
TLIMIT = 8 * 1024 * 1024


def solution(mesh):
    placed = (
        P("angle", "pos", None, None),
        P("angle", "pos", None),
        P(),
        P("angle", None, "pos", None),
        P(),
        P(),
    )
    return jax.shard_map(
        functools.partial(on_device, mesh.shape["angle"], mesh.shape["pos"]),
        mesh=mesh,
        in_specs=placed,
        out_specs=(P("angle", None, "pos", None), P(), P("pos", "angle", None, None)),
        check_vma=False,
    )
```

```python
import functools
import math

import jax
import jax.numpy as jnp
import numpy as np
from jax import lax
from jax.experimental import pallas as pl
from jax.experimental.pallas import tpu as pltpu
from jax.sharding import PartitionSpec as P

MESH = pl.DeviceIdType.MESH
VMEM = pltpu.VMEM
LANES = 128


def split_const(table):
    high = jnp.asarray(table, jnp.float32).astype(jnp.bfloat16)
    low = (jnp.asarray(table, jnp.float32) - high.astype(jnp.float32)).astype(jnp.bfloat16)
    return high, low


def dft_blocks(length):
    ramp = np.arange(length)
    theta = (ramp[:, None] * ramp[None, :] % length) * (2.0 * math.pi / length)
    real = np.cos(theta) / math.sqrt(length)
    imag = -np.sin(theta) / math.sqrt(length)
    left = np.block([[real, -imag], [imag, real]])
    right = np.block([[real, imag], [-imag, real]])
    return np.asarray(left, np.float32), np.asarray(right, np.float32)


def halves(value):
    high = value.astype(jnp.bfloat16)
    return high, (value - high.astype(jnp.float32)).astype(jnp.bfloat16)


def mm(a, b):
    return jnp.dot(a, b, preferred_element_type=jnp.float32)


def left3(table_high, table_low, value):
    high, low = halves(value)
    return mm(table_high, high) + mm(table_high, low) + mm(table_low, high)


def right3(value, table_high, table_low):
    high, low = halves(value)
    return mm(high, table_high) + mm(low, table_high) + mm(high, table_low)


def remote(src, dst, send, recv, axis, target):
    return pltpu.make_async_remote_copy(
        src_ref=src, dst_ref=dst, send_sem=send, recv_sem=recv,
        device_id={axis: target}, device_id_type=MESH,
    )


def flip(me, mask, bits):
    other = 0
    for b in range(bits):
        bit = (me // (1 << b)) % 2
        other = other + (1 << b) * (1 - bit if (mask >> b) & 1 else bit)
    return other


def step_kernel(n_ang, n_pos, size,
                offs_h, obj_h, amp_h, probe_h, index_h, weight_h, ah_h, al_h, bh_h, bl_h,
                newobj, recon, change,
                offs, near, obj, amp, probe, index, weight, ah, al, bh, bl,
                ext, sb, zo, za, zb, accw, acci, accr, grad, from_above, from_below,
                numden, rs, partial, ag, piece, sino, tables, rh, rl,
                in_sem, send_sem, recv_sem, rs_send, rs_recv,
                a2a_send, a2a_recv, ag_send, ag_recv, fin_send, fin_recv):
    me_a = lax.axis_index("angle")
    me = lax.axis_index("pos")
    up, down = lax.rem(me + n_pos - 1, n_pos), lax.rem(me + 1, n_pos)
    tiles, band = obj.shape[1], obj.shape[2]
    width = tiles * LANES
    patch = probe.shape[1]
    half = patch // 2
    count = amp.shape[1]
    ns = sino.shape[1]

    sources = [(offs_h, offs), (probe_h, probe), (amp_h, amp),
               (ah_h, ah), (al_h, al), (bh_h, bh), (bl_h, bl), (index_h, index), (weight_h, weight)]
    sources += [(obj_h.at[0, :, :, pl.ds(t * LANES, LANES)], obj.at[:, t]) for t in range(tiles)]
    loads = [pltpu.make_async_copy(src, dst, in_sem.at[k]) for k, (src, dst) in enumerate(sources)]
    for copy in loads:
        copy.start()
    bits = (n_ang - 1).bit_length()
    order = [1] + list(range(n_ang - 1, 1, -1))
    angle_peers = [flip(me_a, mask, bits) for mask in order]
    pos_peers = [lax.rem(me + d, n_pos) for d in range(1, n_pos)]
    barrier = pltpu.get_barrier_semaphore()
    for peer in pos_peers:
        pl.semaphore_signal(barrier, inc=1, device_id={"pos": peer}, device_id_type=MESH)
    for peer in angle_peers:
        pl.semaphore_signal(barrier, inc=1, device_id={"angle": peer}, device_id_type=MESH)
    loads[0].wait()
    pl.semaphore_wait(barrier, n_ang + n_pos - 2)
    swap = [remote(offs, near.at[0], send_sem.at[0], recv_sem.at[0], "pos", down),
            remote(offs, near.at[1], send_sem.at[1], recv_sem.at[1], "pos", up)]
    for copy in swap:
        copy.start()
    for copy in loads[9:]:
        copy.wait()

    def columns(c, rows, col):
        tile = col // LANES
        after = jnp.minimum(tile + 1, tiles - 1)
        got = jnp.concatenate([obj[c, tile, rows, :], obj[c, after, rows, :]], axis=1)
        return pltpu.roll(got, lax.rem(2 * LANES - lax.rem(col, LANES), 2 * LANES), 1)[:, :patch]

    for j in range(count):
        for c in range(2):
            ext[j // size][j % size, c, half:half + band, :] = columns(c, slice(0, band), offs[1, j])
    zo[...] = jnp.zeros_like(zo)
    za[...] = jnp.zeros_like(za)
    zb[...] = jnp.zeros_like(zb)
    for k, copy in enumerate(swap):
        copy.wait()
    first = []
    groups = [range(g * size, (g + 1) * size) for g in range(count // size)]
    for g, group in enumerate(groups):
        for j in group:
            for c in range(2):
                sb[0, j, c] = columns(c, slice(band - half, band), near[1, 1, j])
                sb[1, j, c] = columns(c, slice(0, half), near[0, 1, j])
        span = pl.ds(g * size, size)
        pair = [
            remote(sb.at[0, span], ext[g].at[:, :, pl.ds(0, half), :],
                   send_sem.at[2 + 6 * g], recv_sem.at[2 + 6 * g], "pos", down),
            remote(sb.at[1, span], ext[g].at[:, :, pl.ds(half + band, half), :],
                   send_sem.at[3 + 6 * g], recv_sem.at[3 + 6 * g], "pos", up),
        ]
        for copy in pair:
            copy.start()
        first.append(pair)

    def spot(row, col, owner):
        return jnp.clip(row - owner * band + half, 0, band), col

    own_at = [spot(offs[0, j], offs[1, j], me) for j in range(count)]
    above_at = [spot(near[0, 0, j], near[0, 1, j], up) for j in range(count)]
    below_at = [spot(near[1, 0, j], near[1, 1, j], down) for j in range(count)]

    def wide(plane, col):
        blank = jnp.zeros((plane.shape[0], LANES), jnp.float32)
        both = jnp.concatenate([plane, blank], axis=1)
        return pltpu.roll(both, lax.rem(col, LANES), 1)

    lead = max(0, band - half)

    def place(acc, buf, first_row, plane, start, rows, col):
        shifted = wide(plane, col)
        where = slice(first_row, first_row + plane.shape[0])
        buf[tiles - 1, where, :] = shifted[:, :LANES]
        buf[tiles, where, :] = shifted[:, LANES:]
        begin = tiles - 1 - col // LANES
        for t in range(tiles):
            acc[t, rows, :] = acc[t, rows, :] + buf[begin + t, pl.ds(start, rows.stop - rows.start), :]

    def place_own(acc, plane, j):
        row, col = own_at[j]
        place(acc, zo, lead, plane, lead + half - row, slice(0, band), col)

    def place_above(acc, plane, j):
        row, col = above_at[j]
        place(acc, za, 0, plane, band - row, slice(0, half), col)

    def place_below(acc, plane, j):
        row, col = below_at[j]
        place(acc, zb, band, plane, band - row, slice(band - half, band), col)

    loads[1].wait()
    p_re, p_im = probe[0], probe[1]
    power = p_re * p_re + p_im * p_im
    accw[...] = jnp.ones_like(accw)
    acci[...] = jnp.zeros_like(acci)
    accr[...] = jnp.zeros_like(accr)
    for j in range(count):
        place_own(accw, power, j)
        place_above(accw, power[half:], j)
        place_below(accw, power[:half], j)
    accw[...] = 1.0 / accw[...]
    tall = 64

    def ramp(step, carry):
        top = pl.multiple_of(step * tall, tall)
        shape = (tall, width)
        differ = lax.broadcasted_iota(jnp.int32, shape, 1) - (
            lax.broadcasted_iota(jnp.int32, shape, 0) + top)
        spread = differ.astype(jnp.float32)
        odd = -1.0 / (jnp.maximum(spread * spread, 1.0) * (math.pi * math.pi))
        value = jnp.where((differ & 1) == 1, odd, jnp.where(differ == 0, 0.25, 0.0))
        rh[pl.ds(top, tall), :], rl[pl.ds(top, tall), :] = halves(value)
        return carry

    lax.fori_loop(0, width // tall, ramp, 0)
    for copy in loads[2:9]:
        copy.wait()
    chunk = tables.shape[2]
    per_row = width // chunk
    zwin = index.shape[1]
    per_angle = zwin * per_row
    deep = 16
    pattern = lax.broadcasted_iota(jnp.int32, (deep, chunk), 0)
    one, zero = jnp.ones((deep, chunk), jnp.bfloat16), jnp.zeros((deep, chunk), jnp.bfloat16)
    pattern = pattern.astype(jnp.int16)

    origins = [me_a] + angle_peers

    def build(k, step, carry):
        a = origins[k]
        z = step // per_row
        lanes = pl.ds(pl.multiple_of(lax.rem(step, per_row) * chunk, chunk), chunk)
        at = jnp.broadcast_to(index[a, pl.ds(z, 1), lanes], (deep, chunk)).astype(jnp.int16)
        for r in range(width // deep):
            hit = at == pattern + jnp.int16(r * deep)
            tables[k * per_angle + step, r * deep:(r + 1) * deep, :] = jnp.where(hit, one, zero)
        return carry

    def build_all(k):
        lax.fori_loop(0, per_angle, functools.partial(build, k), 0)

    for k in range(n_ang):
        build_all(k)
    n_re = jnp.zeros((patch, patch), jnp.float32)
    n_im = n_re
    den = n_re
    second = []
    for g, group in enumerate(groups):
        for copy in first[g]:
            copy.wait()
        q_re, q_im, w_re, w_im = [], [], [], []
        for j in group:
            rows = pl.ds(own_at[j][0], patch)
            re, im = ext[g][j % size, 0, rows, :], ext[g][j % size, 1, rows, :]
            q_re.append(re)
            q_im.append(im)
            w_re.append(p_re * re - p_im * im)
            w_im.append(p_re * im + p_im * re)
        psi = jnp.concatenate([jnp.concatenate(w_re, axis=1), jnp.concatenate(w_im, axis=1)], axis=0)
        mid = left3(ah[...], al[...], psi)
        cells = [slice(n * patch, (n + 1) * patch) for n in range(size)]
        rows = [jnp.concatenate([mid[:patch, cell], mid[patch:, cell]], axis=1) for cell in cells]
        spec = right3(jnp.concatenate(rows, axis=0), bh[...], bl[...])
        fixed = []
        for j, cell in zip(group, cells):
            s_re = spec[cell, :patch]
            s_im = spec[cell, patch:]
            factor = amp[0, j] / jnp.maximum(jnp.sqrt(s_re * s_re + s_im * s_im), 0.5)
            fixed.append(jnp.concatenate([factor * s_re, factor * s_im], axis=1))
        back = right3(jnp.concatenate(fixed, axis=0), ah[...], al[...])
        wide_re = jnp.concatenate([back[cell, :patch] for cell in cells], axis=1)
        wide_im = jnp.concatenate([back[cell, patch:] for cell in cells], axis=1)
        diff = left3(bh[...], bl[...], jnp.concatenate([wide_re, wide_im], axis=0))
        diff = diff - psi
        for n, j in enumerate(group):
            d_re, d_im = diff[:patch, cells[n]], diff[patch:, cells[n]]
            g_re = p_re * d_re + p_im * d_im
            g_im = p_re * d_im - p_im * d_re
            for h in range(2):
                grad[h, j, 0] = g_re[h * half:(h + 1) * half]
                grad[h, j, 1] = g_im[h * half:(h + 1) * half]
            n_re = n_re + (q_re[n] * d_re + q_im[n] * d_im)
            n_im = n_im + (q_re[n] * d_im - q_im[n] * d_re)
            den = den + (q_re[n] * q_re[n] + q_im[n] * q_im[n])
        span = pl.ds(g * size, size)
        pairs = []
        for c in (1, 0):
            k = 4 + 6 * g + 2 * (1 - c)
            pairs.append([
                remote(grad.at[1, span, c], from_above.at[span, c], send_sem.at[k], recv_sem.at[k], "pos", down),
                remote(grad.at[0, span, c], from_below.at[span, c], send_sem.at[k + 1], recv_sem.at[k + 1], "pos", up),
            ])
        for copy in pairs[0] + ([] if g == len(groups) - 1 else pairs[1]):
            copy.start()
        second.append(pairs)
    numden[0] = n_re
    numden[1] = n_im
    numden[2] = den
    pr = patch // n_pos
    scatter = [
        remote(numden.at[:, pl.ds(pl.multiple_of(peer * pr, 8), pr), :], rs.at[d],
               rs_send.at[d], rs_recv.at[d], "pos", peer)
        for d, peer in enumerate(pos_peers)
    ]
    for copy in scatter + second[-1][1]:
        copy.start()

    def whole_patch(j, c):
        return jnp.concatenate([grad[0, j, c], grad[1, j, c]], axis=0)

    for j in range(count):
        place_own(acci, whole_patch(j, 1), j)
    for g, group in enumerate(groups):
        for copy in second[g][0]:
            copy.wait()
        for j in group:
            place_above(acci, from_above[j, 1], j)
            place_below(acci, from_below[j, 1], j)
    for t in range(tiles):
        lanes = slice(t * LANES, (t + 1) * LANES)
        newobj[0, 1, :, lanes] = obj[1, t] + acci[t] * accw[t]
    def project(k, a, lines):
        high, low = halves(lines)
        both = mm(jnp.concatenate([high, low], axis=0), rh[...])
        lines = (both[:ns] + both[ns:] + mm(high, rl[...])) * (math.pi / n_ang)
        high, low = halves(lines)
        next_high, next_low = halves(pltpu.roll(lines, width - 1, 1))
        stack = jnp.concatenate([high, low, next_high, next_low], axis=0)
        for n in range(per_angle):
            z, part = n // per_row, n % per_row
            got = mm(stack, tables[k * per_angle + n])
            lower = got[:ns] + got[ns:2 * ns]
            upper = got[2 * ns:3 * ns] + got[3 * ns:]
            w = weight[pl.ds(a, 1), z, pl.ds(part * chunk, chunk)]
            value = (1.0 - w) * lower + w * upper
            lanes = pl.ds(n * chunk, chunk)
            recon[:, lanes] = value if k == 0 else recon[:, lanes] + value

    across = [
        remote(newobj.at[0, 1, pl.ds(pl.multiple_of(peer * ns, 8), ns), :], sino.at[k],
               a2a_send.at[k], a2a_recv.at[k], "angle", peer)
        for k, peer in enumerate(angle_peers)
    ]
    inner = (me_a >= n_ang // 4) & (me_a < n_ang - n_ang // 4)
    across[0].start()

    @pl.when(inner)
    def _():
        for copy in across[1:-1]:
            copy.start()

    for copy in scatter:
        copy.wait()
    part = numden[:, pl.ds(pl.multiple_of(me * pr, 8), pr), :]
    for d in range(n_pos - 1):
        part = part + rs[d]
    partial[0] = part
    shares = [
        remote(partial.at[b], ag.at[b], ag_send.at[b], ag_recv.at[b], "angle", flip(me_a, 1 << b, bits))
        for b in range(bits)
    ]
    shares[0].start()

    @pl.when(jnp.logical_not(inner))
    def _():
        for copy in across[1:-1]:
            copy.start()

    project(0, me_a, newobj[0, 1, pl.ds(pl.multiple_of(me_a * ns, 8), ns), :])
    for b in range(bits - 1):
        shares[b].wait()
        partial[b + 1] = partial[b] + ag[b]
        shares[b + 1].start()
    across[-1].start()
    for g, group in enumerate(groups):
        for copy in second[g][1]:
            copy.wait()
        for j in group:
            place_own(accr, whole_patch(j, 0), j)
            place_above(accr, from_above[j, 0], j)
            place_below(accr, from_below[j, 0], j)
    for t in range(tiles):
        lanes = slice(t * LANES, (t + 1) * LANES)
        newobj[0, 0, :, lanes] = obj[0, t] + accr[t] * accw[t]
    shares[-1].wait()
    total = partial[bits - 1] + ag[bits - 1]
    mine = pl.ds(pl.multiple_of(me * pr, 8), pr)
    for c in range(2):
        value = total[c] / (total[2] + 1.0)
        piece[c] = value
        change[c, mine, :] = value
    spread = [
        remote(piece, change.at[:, mine, :], fin_send.at[d], fin_recv.at[d], "pos", peer)
        for d, peer in enumerate(pos_peers)
    ]
    for copy in spread:
        copy.start()
    for k, peer in enumerate(angle_peers):
        across[k].wait()
        project(k + 1, peer, sino[k])
    for copy in spread:
        copy.wait()


def tail_kernel(newobj, recon, change, probe, out_obj, out_probe, out_recon, sem):
    copy = pltpu.make_async_copy(newobj, out_obj, sem.at[0])
    copy.start()
    out_probe[...] = probe[...] + change[...]
    width = out_recon.shape[3]
    for s in range(out_recon.shape[1]):
        for z in range(out_recon.shape[2]):
            out_recon[0, s, z:z + 1, :] = recon[s:s + 1, z * width:(z + 1) * width]
    copy.wait()


def on_device(n_ang, n_pos, amplitude, offsets, probe_field, object_field, interp_index, interp_weight):
    band = object_field.shape[2]
    width = object_field.shape[3]
    patch = probe_field.shape[1]
    half = patch // 2
    count = offsets.shape[1]
    tiles = width // LANES
    f32, i32, bf16 = jnp.float32, jnp.int32, jnp.bfloat16
    n_z = interp_index.shape[1]
    chunk = min(512, width)
    tables = n_ang * n_z * (width // chunk)
    size = 2 if count % 2 == 0 else count
    left, right = dft_blocks(patch)
    ah, al = split_const(left)
    bh, bl = split_const(right)
    vmem = pl.BlockSpec(memory_space=VMEM)
    hbm = pl.BlockSpec(memory_space=pl.ANY)
    sds = jax.ShapeDtypeStruct
    dma = pltpu.SemaphoreType.DMA
    total = n_z * width
    ns = band // n_ang
    pr = patch // n_pos
    lead = max(0, band - half)
    ext = 2 * tiles
    table = VMEM((2 * patch, 2 * patch), bf16)
    half_shape = (count, 2, half, patch)
    bits = (n_ang - 1).bit_length()
    links = 2 + 6 * (count // size)
    newobj, recon, change = pl.pallas_call(
        functools.partial(step_kernel, n_ang, n_pos, size),
        out_shape=(VMEM(object_field.shape, f32), VMEM((ns, total), f32), VMEM(probe_field.shape, f32)),
        in_specs=[hbm] * 10,
        out_specs=(vmem,) * 3,
        scratch_shapes=[
            pltpu.SMEM((2, count), i32), pltpu.SMEM((2, 2, count), i32),
            VMEM((2, tiles, band, LANES), f32), VMEM(amplitude.shape, f32), VMEM(probe_field.shape, f32),
            VMEM(interp_index.shape, i32), VMEM(interp_weight.shape, f32),
            table, table, table, table,
            [VMEM((size, 2, band + patch, patch), f32)] * (count // size), VMEM((2,) + half_shape, f32),
            VMEM((ext, lead + half + band, LANES), f32),
            VMEM((ext, half + band, LANES), f32), VMEM((ext, half + band, LANES), f32),
            VMEM((tiles, band, LANES), f32), VMEM((tiles, band, LANES), f32), VMEM((tiles, band, LANES), f32),
            VMEM((2,) + half_shape, f32), VMEM(half_shape, f32), VMEM(half_shape, f32),
            VMEM((3, patch, patch), f32), VMEM((n_pos - 1, 3, pr, patch), f32),
            VMEM((bits, 3, pr, patch), f32), VMEM((bits, 3, pr, patch), f32), VMEM((2, pr, patch), f32),
            VMEM((n_ang - 1, ns, width), f32),
            VMEM((tables, width, chunk), bf16), VMEM((width, width), bf16), VMEM((width, width), bf16),
            dma((9 + tiles,)), dma((links,)), dma((links,)), dma((n_pos - 1,)), dma((n_pos - 1,)),
            dma((n_ang - 1,)), dma((n_ang - 1,)), dma((bits,)), dma((bits,)),
            dma((n_pos - 1,)), dma((n_pos - 1,)),
        ],
        compiler_params=pltpu.CompilerParams(
            collective_id=0, has_side_effects=True, vmem_limit_bytes=KLIMIT),
        name="step",
    )(*(pltpu.with_memory_space_constraint(x, pltpu.HBM) for x in (
        jnp.transpose(offsets[0]), object_field, amplitude, probe_field, interp_index, interp_weight,
        ah, al, bh, bl)))
    out = pl.pallas_call(
        tail_kernel,
        out_shape=(sds(object_field.shape, f32), sds(probe_field.shape, f32), sds((1, ns, n_z, width), f32)),
        in_specs=[vmem] * 4,
        out_specs=(hbm, vmem, vmem),
        scratch_shapes=[dma((1,))],
        compiler_params=pltpu.CompilerParams(vmem_limit_bytes=TLIMIT),
        name="tail",
    )(newobj, recon, change, probe_field)
    return tuple(out)


KLIMIT = 48 * 1024 * 1024
TLIMIT = 8 * 1024 * 1024


def solution(mesh):
    placed = (
        P("angle", "pos", None, None),
        P("angle", "pos", None),
        P(),
        P("angle", None, "pos", None),
        P(),
        P(),
    )
    return jax.shard_map(
        functools.partial(on_device, mesh.shape["angle"], mesh.shape["pos"]),
        mesh=mesh,
        in_specs=placed,
        out_specs=(P("angle", None, "pos", None), P(), P("pos", "angle", None, None)),
        check_vma=False,
    )
```

```python
import functools
import math

import jax
import jax.numpy as jnp
import numpy as np
from jax import lax
from jax.experimental import pallas as pl
from jax.experimental.pallas import tpu as pltpu
from jax.sharding import PartitionSpec as P

MESH = pl.DeviceIdType.MESH
VMEM = pltpu.VMEM
LANES = 128


def split_const(table):
    high = jnp.asarray(table, jnp.float32).astype(jnp.bfloat16)
    low = (jnp.asarray(table, jnp.float32) - high.astype(jnp.float32)).astype(jnp.bfloat16)
    return high, low


def dft_blocks(length):
    ramp = np.arange(length)
    theta = (ramp[:, None] * ramp[None, :] % length) * (2.0 * math.pi / length)
    real = np.cos(theta) / math.sqrt(length)
    imag = -np.sin(theta) / math.sqrt(length)
    left = np.block([[real, -imag], [imag, real]])
    right = np.block([[real, imag], [-imag, real]])
    return np.asarray(left, np.float32), np.asarray(right, np.float32)


def halves(value):
    high = value.astype(jnp.bfloat16)
    return high, (value - high.astype(jnp.float32)).astype(jnp.bfloat16)


def mm(a, b):
    return jnp.dot(a, b, preferred_element_type=jnp.float32)


def left3(table_high, table_low, value):
    high, low = halves(value)
    return mm(table_high, high) + mm(table_high, low) + mm(table_low, high)


def right3(value, table_high, table_low):
    high, low = halves(value)
    return mm(high, table_high) + mm(low, table_high) + mm(high, table_low)


def remote(src, dst, send, recv, axis, target):
    return pltpu.make_async_remote_copy(
        src_ref=src, dst_ref=dst, send_sem=send, recv_sem=recv,
        device_id={axis: target}, device_id_type=MESH,
    )


def flip(me, mask, bits):
    other = 0
    for b in range(bits):
        bit = (me // (1 << b)) % 2
        other = other + (1 << b) * (1 - bit if (mask >> b) & 1 else bit)
    return other


def step_kernel(n_ang, n_pos, size,
                offs_h, obj_h, amp_h, probe_h, index_h, weight_h, ah_h, al_h, bh_h, bl_h,
                newobj, recon, change,
                offs, near, obj, amp, probe, index, weight, ah, al, bh, bl,
                ext, sb, zo, za, zb, accw, acci, accr, grad, from_above, from_below,
                numden, rs, partial, ag, piece, sino, tables, rh, rl,
                in_sem, send_sem, recv_sem, rs_send, rs_recv,
                a2a_send, a2a_recv, ag_send, ag_recv, fin_send, fin_recv):
    me_a = lax.axis_index("angle")
    me = lax.axis_index("pos")
    up, down = lax.rem(me + n_pos - 1, n_pos), lax.rem(me + 1, n_pos)
    tiles, band = obj.shape[1], obj.shape[2]
    width = tiles * LANES
    patch = probe.shape[1]
    half = patch // 2
    count = amp.shape[1]
    ns = sino.shape[1]

    sources = [(offs_h, offs), (probe_h, probe), (amp_h, amp),
               (ah_h, ah), (al_h, al), (bh_h, bh), (bl_h, bl), (index_h, index), (weight_h, weight)]
    sources += [(obj_h.at[0, :, :, pl.ds(t * LANES, LANES)], obj.at[:, t]) for t in range(tiles)]
    loads = [pltpu.make_async_copy(src, dst, in_sem.at[k]) for k, (src, dst) in enumerate(sources)]
    for copy in loads:
        copy.start()
    bits = (n_ang - 1).bit_length()
    order = [1] + list(range(n_ang - 1, 1, -1))
    angle_peers = [flip(me_a, mask, bits) for mask in order]
    pos_peers = [lax.rem(me + d, n_pos) for d in range(1, n_pos)]
    barrier = pltpu.get_barrier_semaphore()
    for peer in pos_peers:
        pl.semaphore_signal(barrier, inc=1, device_id={"pos": peer}, device_id_type=MESH)
    for peer in angle_peers:
        pl.semaphore_signal(barrier, inc=1, device_id={"angle": peer}, device_id_type=MESH)
    loads[0].wait()
    pl.semaphore_wait(barrier, n_ang + n_pos - 2)
    swap = [remote(offs, near.at[0], send_sem.at[0], recv_sem.at[0], "pos", down),
            remote(offs, near.at[1], send_sem.at[1], recv_sem.at[1], "pos", up)]
    for copy in swap:
        copy.start()
    for copy in loads[9:]:
        copy.wait()

    def columns(c, rows, col):
        tile = col // LANES
        after = jnp.minimum(tile + 1, tiles - 1)
        got = jnp.concatenate([obj[c, tile, rows, :], obj[c, after, rows, :]], axis=1)
        return pltpu.roll(got, lax.rem(2 * LANES - lax.rem(col, LANES), 2 * LANES), 1)[:, :patch]

    for j in range(count):
        for c in range(2):
            ext[j // size][j % size, c, half:half + band, :] = columns(c, slice(0, band), offs[1, j])
    zo[...] = jnp.zeros_like(zo)
    za[...] = jnp.zeros_like(za)
    zb[...] = jnp.zeros_like(zb)
    for k, copy in enumerate(swap):
        copy.wait()
    first = []
    groups = [range(g * size, (g + 1) * size) for g in range(count // size)]
    for g, group in enumerate(groups):
        for j in group:
            for c in range(2):
                sb[0, j, c] = columns(c, slice(band - half, band), near[1, 1, j])
                sb[1, j, c] = columns(c, slice(0, half), near[0, 1, j])
        span = pl.ds(g * size, size)
        pair = [
            remote(sb.at[0, span], ext[g].at[:, :, pl.ds(0, half), :],
                   send_sem.at[2 + 6 * g], recv_sem.at[2 + 6 * g], "pos", down),
            remote(sb.at[1, span], ext[g].at[:, :, pl.ds(half + band, half), :],
                   send_sem.at[3 + 6 * g], recv_sem.at[3 + 6 * g], "pos", up),
        ]
        for copy in pair:
            copy.start()
        first.append(pair)

    def spot(row, col, owner):
        return jnp.clip(row - owner * band + half, 0, band), col

    own_at = [spot(offs[0, j], offs[1, j], me) for j in range(count)]
    above_at = [spot(near[0, 0, j], near[0, 1, j], up) for j in range(count)]
    below_at = [spot(near[1, 0, j], near[1, 1, j], down) for j in range(count)]

    def wide(plane, col):
        blank = jnp.zeros((plane.shape[0], LANES), jnp.float32)
        both = jnp.concatenate([plane, blank], axis=1)
        return pltpu.roll(both, lax.rem(col, LANES), 1)

    lead = max(0, band - half)

    def place(acc, buf, first_row, plane, start, rows, col):
        shifted = wide(plane, col)
        where = slice(first_row, first_row + plane.shape[0])
        buf[tiles - 1, where, :] = shifted[:, :LANES]
        buf[tiles, where, :] = shifted[:, LANES:]
        begin = tiles - 1 - col // LANES
        for t in range(tiles):
            acc[t, rows, :] = acc[t, rows, :] + buf[begin + t, pl.ds(start, rows.stop - rows.start), :]

    def place_own(acc, plane, j):
        row, col = own_at[j]
        place(acc, zo, lead, plane, lead + half - row, slice(0, band), col)

    def place_above(acc, plane, j):
        row, col = above_at[j]
        place(acc, za, 0, plane, band - row, slice(0, half), col)

    def place_below(acc, plane, j):
        row, col = below_at[j]
        place(acc, zb, band, plane, band - row, slice(band - half, band), col)

    loads[1].wait()
    p_re, p_im = probe[0], probe[1]
    power = p_re * p_re + p_im * p_im
    accw[...] = jnp.ones_like(accw)
    acci[...] = jnp.zeros_like(acci)
    accr[...] = jnp.zeros_like(accr)
    for j in range(count):
        place_own(accw, power, j)
        place_above(accw, power[half:], j)
        place_below(accw, power[:half], j)
    accw[...] = 1.0 / accw[...]
    tall = 64

    def ramp(step, carry):
        top = pl.multiple_of(step * tall, tall)
        shape = (tall, width)
        differ = lax.broadcasted_iota(jnp.int32, shape, 1) - (
            lax.broadcasted_iota(jnp.int32, shape, 0) + top)
        spread = differ.astype(jnp.float32)
        odd = -1.0 / (jnp.maximum(spread * spread, 1.0) * (math.pi * math.pi))
        value = jnp.where((differ & 1) == 1, odd, jnp.where(differ == 0, 0.25, 0.0))
        rh[pl.ds(top, tall), :], rl[pl.ds(top, tall), :] = halves(value)
        return carry

    lax.fori_loop(0, width // tall, ramp, 0)
    for copy in loads[2:9]:
        copy.wait()
    chunk = tables.shape[2]
    per_row = width // chunk
    zwin = index.shape[1]
    per_angle = zwin * per_row
    deep = 16
    pattern = lax.broadcasted_iota(jnp.int32, (deep, chunk), 0)
    one, zero = jnp.ones((deep, chunk), jnp.bfloat16), jnp.zeros((deep, chunk), jnp.bfloat16)
    pattern = pattern.astype(jnp.int16)

    origins = [me_a] + angle_peers

    def build(k, step, carry):
        a = origins[k]
        z = step // per_row
        lanes = pl.ds(pl.multiple_of(lax.rem(step, per_row) * chunk, chunk), chunk)
        at = jnp.broadcast_to(index[a, pl.ds(z, 1), lanes], (deep, chunk)).astype(jnp.int16)
        for r in range(width // deep):
            hit = at == pattern + jnp.int16(r * deep)
            tables[k * per_angle + step, r * deep:(r + 1) * deep, :] = jnp.where(hit, one, zero)
        return carry

    def build_all(k):
        lax.fori_loop(0, per_angle, functools.partial(build, k), 0)

    for k in range(n_ang):
        build_all(k)
    n_re = jnp.zeros((patch, patch), jnp.float32)
    n_im = n_re
    den = n_re
    second = []
    for g, group in enumerate(groups):
        for copy in first[g]:
            copy.wait()
        q_re, q_im, w_re, w_im = [], [], [], []
        for j in group:
            rows = pl.ds(own_at[j][0], patch)
            re, im = ext[g][j % size, 0, rows, :], ext[g][j % size, 1, rows, :]
            q_re.append(re)
            q_im.append(im)
            w_re.append(p_re * re - p_im * im)
            w_im.append(p_re * im + p_im * re)
        psi = jnp.concatenate([jnp.concatenate(w_re, axis=1), jnp.concatenate(w_im, axis=1)], axis=0)
        mid = left3(ah[...], al[...], psi)
        cells = [slice(n * patch, (n + 1) * patch) for n in range(size)]
        rows = [jnp.concatenate([mid[:patch, cell], mid[patch:, cell]], axis=1) for cell in cells]
        spec = right3(jnp.concatenate(rows, axis=0), bh[...], bl[...])
        fixed = []
        for j, cell in zip(group, cells):
            s_re = spec[cell, :patch]
            s_im = spec[cell, patch:]
            factor = amp[0, j] / jnp.maximum(jnp.sqrt(s_re * s_re + s_im * s_im), 0.5)
            fixed.append(jnp.concatenate([factor * s_re, factor * s_im], axis=1))
        back = right3(jnp.concatenate(fixed, axis=0), ah[...], al[...])
        wide_re = jnp.concatenate([back[cell, :patch] for cell in cells], axis=1)
        wide_im = jnp.concatenate([back[cell, patch:] for cell in cells], axis=1)
        diff = left3(bh[...], bl[...], jnp.concatenate([wide_re, wide_im], axis=0))
        diff = diff - psi
        for n, j in enumerate(group):
            d_re, d_im = diff[:patch, cells[n]], diff[patch:, cells[n]]
            g_re = p_re * d_re + p_im * d_im
            g_im = p_re * d_im - p_im * d_re
            for h in range(2):
                grad[h, j, 0] = g_re[h * half:(h + 1) * half]
                grad[h, j, 1] = g_im[h * half:(h + 1) * half]
            n_re = n_re + (q_re[n] * d_re + q_im[n] * d_im)
            n_im = n_im + (q_re[n] * d_im - q_im[n] * d_re)
            den = den + (q_re[n] * q_re[n] + q_im[n] * q_im[n])
        span = pl.ds(g * size, size)
        pairs = []
        for c in (1, 0):
            k = 4 + 6 * g + 2 * (1 - c)
            pairs.append([
                remote(grad.at[1, span, c], from_above.at[span, c], send_sem.at[k], recv_sem.at[k], "pos", down),
                remote(grad.at[0, span, c], from_below.at[span, c], send_sem.at[k + 1], recv_sem.at[k + 1], "pos", up),
            ])
        for copy in pairs[0] + ([] if g == len(groups) - 1 else pairs[1]):
            copy.start()
        second.append(pairs)
    numden[0] = n_re
    numden[1] = n_im
    numden[2] = den
    pr = patch // n_pos
    scatter = [
        remote(numden.at[:, pl.ds(pl.multiple_of(peer * pr, 8), pr), :], rs.at[d],
               rs_send.at[d], rs_recv.at[d], "pos", peer)
        for d, peer in enumerate(pos_peers)
    ]
    for copy in scatter + second[-1][1]:
        copy.start()

    def whole_patch(j, c):
        return jnp.concatenate([grad[0, j, c], grad[1, j, c]], axis=0)

    for j in range(count):
        place_own(acci, whole_patch(j, 1), j)
    for g, group in enumerate(groups):
        for copy in second[g][0]:
            copy.wait()
        for j in group:
            place_above(acci, from_above[j, 1], j)
            place_below(acci, from_below[j, 1], j)
    for t in range(tiles):
        lanes = slice(t * LANES, (t + 1) * LANES)
        newobj[0, 1, :, lanes] = obj[1, t] + acci[t] * accw[t]
    def project(k, a, lines):
        high, low = halves(lines)
        both = mm(jnp.concatenate([high, low], axis=0), rh[...])
        lines = (both[:ns] + both[ns:] + mm(high, rl[...])) * (math.pi / n_ang)
        high, low = halves(lines)
        next_high, next_low = halves(pltpu.roll(lines, width - 1, 1))
        stack = jnp.concatenate([high, low, next_high, next_low], axis=0)
        for n in range(per_angle):
            z, part = n // per_row, n % per_row
            got = mm(stack, tables[k * per_angle + n])
            lower = got[:ns] + got[ns:2 * ns]
            upper = got[2 * ns:3 * ns] + got[3 * ns:]
            w = weight[pl.ds(a, 1), z, pl.ds(part * chunk, chunk)]
            value = (1.0 - w) * lower + w * upper
            lanes = pl.ds(n * chunk, chunk)
            recon[:, lanes] = value if k == 0 else recon[:, lanes] + value

    across = [
        remote(newobj.at[0, 1, pl.ds(pl.multiple_of(peer * ns, 8), ns), :], sino.at[k],
               a2a_send.at[k], a2a_recv.at[k], "angle", peer)
        for k, peer in enumerate(angle_peers)
    ]
    inner = (me_a >= n_ang // 4) & (me_a < n_ang - n_ang // 4)
    across[0].start()

    @pl.when(inner)
    def _():
        for copy in across[1:-1]:
            copy.start()

    for copy in scatter:
        copy.wait()
    part = numden[:, pl.ds(pl.multiple_of(me * pr, 8), pr), :]
    for d in range(n_pos - 1):
        part = part + rs[d]
    partial[0] = part
    shares = [
        remote(partial.at[b], ag.at[b], ag_send.at[b], ag_recv.at[b], "angle", flip(me_a, 1 << b, bits))
        for b in range(bits)
    ]
    shares[0].start()

    @pl.when(jnp.logical_not(inner))
    def _():
        for copy in across[1:-1]:
            copy.start()

    project(0, me_a, newobj[0, 1, pl.ds(pl.multiple_of(me_a * ns, 8), ns), :])
    for b in range(bits - 1):
        shares[b].wait()
        partial[b + 1] = partial[b] + ag[b]
        shares[b + 1].start()
    across[-1].start()
    for g, group in enumerate(groups):
        for copy in second[g][1]:
            copy.wait()
        for j in group:
            place_own(accr, whole_patch(j, 0), j)
            place_above(accr, from_above[j, 0], j)
            place_below(accr, from_below[j, 0], j)
    for t in range(tiles):
        lanes = slice(t * LANES, (t + 1) * LANES)
        newobj[0, 0, :, lanes] = obj[0, t] + accr[t] * accw[t]
    shares[-1].wait()
    total = partial[bits - 1] + ag[bits - 1]
    mine = pl.ds(pl.multiple_of(me * pr, 8), pr)
    for c in range(2):
        value = total[c] / (total[2] + 1.0)
        piece[c] = value
        change[c, mine, :] = value
    spread = [
        remote(piece, change.at[:, mine, :], fin_send.at[d], fin_recv.at[d], "pos", peer)
        for d, peer in enumerate(pos_peers)
    ]
    for copy in spread:
        copy.start()
    for k, peer in enumerate(angle_peers):
        across[k].wait()
        project(k + 1, peer, sino[k])
    for copy in spread:
        copy.wait()


def slice_kernel(n_ang, n_pos, size,
                 offs_h, obj_h, amp_h, probe_h, index_h, weight_h, ah_h, al_h, bh_h, bl_h,
                 newobj, recon, change,
                 offs, near, far, farn, obj, amp, probe, index, weight, ah, al, bh, bl,
                 ext, sb, zo, za, zb, zq, accw, acci, accr, grad, from_above, from_below,
                 twice, blk, orx, rx, nrx, lw, lg,
                 numden, rs, partial, ag, piece, tables, rh, rl,
                 in_sem, send_sem, recv_sem, rs_send, rs_recv, far_send, far_recv, farn_send, farn_recv,
                 o_send, o_recv, z_send, z_recv, f_send, f_recv, ag_send, ag_recv, fin_send, fin_recv):
    me_a = lax.axis_index("angle")
    me = lax.axis_index("pos")
    up, down = lax.rem(me + n_pos - 1, n_pos), lax.rem(me + 1, n_pos)
    tiles, band = obj.shape[1], obj.shape[2]
    width = tiles * LANES
    patch = probe.shape[1]
    half = patch // 2
    count = amp.shape[1]
    ns = orx.shape[2]
    side = (me_a * ns) // half
    ahead = lax.rem(me + n_pos + 1 - 2 * side, n_pos)
    behind = lax.rem(me + n_pos - 1 + 2 * side, n_pos)

    sources = [(offs_h, offs), (probe_h, probe), (amp_h, amp),
               (ah_h, ah), (al_h, al), (bh_h, bh), (bl_h, bl), (index_h, index), (weight_h, weight)]
    sources += [(obj_h.at[0, :, :, pl.ds(t * LANES, LANES)], obj.at[:, t]) for t in range(tiles)]
    loads = [pltpu.make_async_copy(src, dst, in_sem.at[k]) for k, (src, dst) in enumerate(sources)]
    for copy in loads:
        copy.start()
    bits = (n_ang - 1).bit_length()
    order = [1] + list(range(n_ang - 1, 1, -1))
    angle_peers = [flip(me_a, mask, bits) for mask in order]
    pos_peers = [lax.rem(me + d, n_pos) for d in range(1, n_pos)]
    barrier = pltpu.get_barrier_semaphore()
    for peer in pos_peers:
        pl.semaphore_signal(barrier, inc=1, device_id={"pos": peer}, device_id_type=MESH)
    for peer in angle_peers:
        pl.semaphore_signal(barrier, inc=1, device_id={"angle": peer}, device_id_type=MESH)
    loads[0].wait()
    pl.semaphore_wait(barrier, n_ang + n_pos - 2)
    swap = [remote(offs, near.at[0], send_sem.at[0], recv_sem.at[0], "pos", down),
            remote(offs, near.at[1], send_sem.at[1], recv_sem.at[1], "pos", up)]
    reach = [remote(offs, far.at[n], far_send.at[n], far_recv.at[n], "angle", peer)
             for n, peer in enumerate(angle_peers)]
    for copy in swap + reach:
        copy.start()
    for copy in loads[9:]:
        copy.wait()
    early = [remote(obj.at[1, :, pl.ds(pl.multiple_of(peer * ns, 8), ns), :], orx.at[n],
                    o_send.at[n], o_recv.at[n], "angle", peer)
             for n, peer in enumerate(angle_peers)]
    for copy in early:
        copy.start()

    def columns(c, rows, col):
        tile = col // LANES
        after = jnp.minimum(tile + 1, tiles - 1)
        got = jnp.concatenate([obj[c, tile, rows, :], obj[c, after, rows, :]], axis=1)
        return pltpu.roll(got, lax.rem(2 * LANES - lax.rem(col, LANES), 2 * LANES), 1)[:, :patch]

    for j in range(count):
        for c in range(2):
            ext[j // size][j % size, c, half:half + band, :] = columns(c, slice(0, band), offs[1, j])
    zo[...] = jnp.zeros_like(zo)
    za[...] = jnp.zeros_like(za)
    zb[...] = jnp.zeros_like(zb)
    zq[...] = jnp.zeros_like(zq)
    lg[...] = jnp.zeros_like(lg)
    lw[...] = jnp.ones_like(lw)
    for k, copy in enumerate(swap):
        copy.wait()
    first = []
    groups = [range(g * size, (g + 1) * size) for g in range(count // size)]
    for g, group in enumerate(groups):
        for j in group:
            for c in range(2):
                sb[0, j, c] = columns(c, slice(band - half, band), near[1, 1, j])
                sb[1, j, c] = columns(c, slice(0, half), near[0, 1, j])
        span = pl.ds(g * size, size)
        pair = [
            remote(sb.at[0, span], ext[g].at[:, :, pl.ds(0, half), :],
                   send_sem.at[2 + 6 * g], recv_sem.at[2 + 6 * g], "pos", down),
            remote(sb.at[1, span], ext[g].at[:, :, pl.ds(half + band, half), :],
                   send_sem.at[3 + 6 * g], recv_sem.at[3 + 6 * g], "pos", up),
        ]
        for copy in pair:
            copy.start()
        first.append(pair)
    relay = [remote(far.at[n], farn.at[n], farn_send.at[n], farn_recv.at[n], "pos", ahead)
             for n in range(n_ang - 1)]
    for n in range(n_ang - 1):
        reach[n].wait()
        relay[n].start()

    def spot(row, col, owner):
        return jnp.clip(row - owner * band + half, 0, band), col

    own_at = [spot(offs[0, j], offs[1, j], me) for j in range(count)]
    above_at = [spot(near[0, 0, j], near[0, 1, j], up) for j in range(count)]
    below_at = [spot(near[1, 0, j], near[1, 1, j], down) for j in range(count)]

    def wide(plane, col):
        blank = jnp.zeros((plane.shape[0], LANES), jnp.float32)
        both = jnp.concatenate([plane, blank], axis=1)
        return pltpu.roll(both, lax.rem(col, LANES), 1)

    lead = max(0, band - half)

    def place(acc, buf, first_row, plane, start, rows, col):
        shifted = wide(plane, col)
        where = slice(first_row, first_row + plane.shape[0])
        buf[tiles - 1, where, :] = shifted[:, :LANES]
        buf[tiles, where, :] = shifted[:, LANES:]
        begin = tiles - 1 - col // LANES
        for t in range(tiles):
            acc[t, rows, :] = acc[t, rows, :] + buf[begin + t, pl.ds(start, rows.stop - rows.start), :]

    def place_own(acc, plane, j):
        row, col = own_at[j]
        place(acc, zo, lead, plane, lead + half - row, slice(0, band), col)

    def place_above(acc, plane, j):
        row, col = above_at[j]
        place(acc, za, 0, plane, band - row, slice(0, half), col)

    def place_below(acc, plane, j):
        row, col = below_at[j]
        place(acc, zb, band, plane, band - row, slice(band - half, band), col)

    loads[1].wait()
    p_re, p_im = probe[0], probe[1]
    power = p_re * p_re + p_im * p_im
    accw[...] = jnp.ones_like(accw)
    acci[...] = jnp.zeros_like(acci)
    accr[...] = jnp.zeros_like(accr)
    for j in range(count):
        place_own(accw, power, j)
        place_above(accw, power[half:], j)
        place_below(accw, power[:half], j)
    accw[...] = 1.0 / accw[...]
    tall = 64

    def ramp(step, carry):
        top = pl.multiple_of(step * tall, tall)
        shape = (tall, width)
        differ = lax.broadcasted_iota(jnp.int32, shape, 1) - (
            lax.broadcasted_iota(jnp.int32, shape, 0) + top)
        spread = differ.astype(jnp.float32)
        odd = -1.0 / (jnp.maximum(spread * spread, 1.0) * (math.pi * math.pi))
        value = jnp.where((differ & 1) == 1, odd, jnp.where(differ == 0, 0.25, 0.0))
        rh[pl.ds(top, tall), :], rl[pl.ds(top, tall), :] = halves(value)
        return carry

    lax.fori_loop(0, width // tall, ramp, 0)
    for copy in loads[2:9]:
        copy.wait()
    chunk = tables.shape[2]
    per_row = width // chunk
    zwin = index.shape[1]
    per_angle = zwin * per_row
    deep = 16
    pattern = lax.broadcasted_iota(jnp.int32, (deep, chunk), 0)
    one, zero = jnp.ones((deep, chunk), jnp.bfloat16), jnp.zeros((deep, chunk), jnp.bfloat16)
    pattern = pattern.astype(jnp.int16)

    origins = [me_a] + angle_peers

    def build(k, step, carry):
        a = origins[k]
        z = step // per_row
        lanes = pl.ds(pl.multiple_of(lax.rem(step, per_row) * chunk, chunk), chunk)
        at = jnp.broadcast_to(index[a, pl.ds(z, 1), lanes], (deep, chunk)).astype(jnp.int16)
        for r in range(width // deep):
            hit = at == pattern + jnp.int16(r * deep)
            tables[k * per_angle + step, r * deep:(r + 1) * deep, :] = jnp.where(hit, one, zero)
        return carry

    def build_all(k):
        lax.fori_loop(0, per_angle, functools.partial(build, k), 0)

    for k in range(n_ang):
        build_all(k)
    n_re = jnp.zeros((patch, patch), jnp.float32)
    n_im = n_re
    den = n_re
    second, outward, forward = [], [], []
    for g, group in enumerate(groups):
        for copy in first[g]:
            copy.wait()
        q_re, q_im, w_re, w_im = [], [], [], []
        for j in group:
            rows = pl.ds(own_at[j][0], patch)
            re, im = ext[g][j % size, 0, rows, :], ext[g][j % size, 1, rows, :]
            q_re.append(re)
            q_im.append(im)
            w_re.append(p_re * re - p_im * im)
            w_im.append(p_re * im + p_im * re)
        psi = jnp.concatenate([jnp.concatenate(w_re, axis=1), jnp.concatenate(w_im, axis=1)], axis=0)
        mid = left3(ah[...], al[...], psi)
        cells = [slice(n * patch, (n + 1) * patch) for n in range(size)]
        rows = [jnp.concatenate([mid[:patch, cell], mid[patch:, cell]], axis=1) for cell in cells]
        spec = right3(jnp.concatenate(rows, axis=0), bh[...], bl[...])
        fixed = []
        for j, cell in zip(group, cells):
            s_re = spec[cell, :patch]
            s_im = spec[cell, patch:]
            factor = amp[0, j] / jnp.maximum(jnp.sqrt(s_re * s_re + s_im * s_im), 0.5)
            fixed.append(jnp.concatenate([factor * s_re, factor * s_im], axis=1))
        back = right3(jnp.concatenate(fixed, axis=0), ah[...], al[...])
        wide_re = jnp.concatenate([back[cell, :patch] for cell in cells], axis=1)
        wide_im = jnp.concatenate([back[cell, patch:] for cell in cells], axis=1)
        diff = left3(bh[...], bl[...], jnp.concatenate([wide_re, wide_im], axis=0))
        diff = diff - psi
        for n, j in enumerate(group):
            d_re, d_im = diff[:patch, cells[n]], diff[patch:, cells[n]]
            g_re = p_re * d_re + p_im * d_im
            g_im = p_re * d_im - p_im * d_re
            twice[n, :patch] = g_im
            twice[n, patch:] = g_im
            blk[j] = twice[n, pl.ds(lax.rem(2 * band - (offs[0, j] - me * band), band), band), :]
            for h in range(2):
                grad[h, j, 0] = g_re[h * half:(h + 1) * half]
                grad[h, j, 1] = g_im[h * half:(h + 1) * half]
            n_re = n_re + (q_re[n] * d_re + q_im[n] * d_im)
            n_im = n_im + (q_re[n] * d_im - q_im[n] * d_re)
            den = den + (q_re[n] * q_re[n] + q_im[n] * q_im[n])
        span = pl.ds(g * size, size)
        out = [remote(blk.at[span, pl.ds(pl.multiple_of(peer * ns, 8), ns), :], rx.at[n, span],
                      z_send.at[n, g], z_recv.at[n, g], "angle", peer)
               for n, peer in enumerate(angle_peers)]
        mine = remote(blk.at[span, pl.ds(pl.multiple_of(me_a * ns, 8), ns), :], nrx.at[0, span],
                      f_send.at[0, g], f_recv.at[0, g], "pos", ahead)
        for copy in out + [mine]:
            copy.start()
        outward.append(out)
        forward.append([mine])
        pairs = []
        for c in (1, 0):
            k = 4 + 6 * g + 2 * (1 - c)
            pairs.append([
                remote(grad.at[1, span, c], from_above.at[span, c], send_sem.at[k], recv_sem.at[k], "pos", down),
                remote(grad.at[0, span, c], from_below.at[span, c], send_sem.at[k + 1], recv_sem.at[k + 1], "pos", up),
            ])
        for copy in pairs[0] + ([] if g == len(groups) - 1 else pairs[1]):
            copy.start()
        second.append(pairs)
    numden[0] = n_re
    numden[1] = n_im
    numden[2] = den
    pr = patch // n_pos
    scatter = [
        remote(numden.at[:, pl.ds(pl.multiple_of(peer * pr, 8), pr), :], rs.at[d],
               rs_send.at[d], rs_recv.at[d], "pos", peer)
        for d, peer in enumerate(pos_peers)
    ]
    for copy in scatter:
        copy.start()

    def whole_patch(j, c):
        return jnp.concatenate([grad[0, j, c], grad[1, j, c]], axis=0)

    places = [offs] + [far.at[n] for n in range(n_ang - 1)]
    behinds = [near.at[side]] + [farn.at[n] for n in range(n_ang - 1)]
    slot = lax.broadcasted_iota(jnp.int32, (ns, LANES), 0) + me_a * ns

    def mark(row, beside):
        if beside:
            return jnp.where(side == 0, (slot < row).astype(jnp.float32), (slot >= row + band).astype(jnp.float32))
        return ((slot >= row) & (slot < row + band)).astype(jnp.float32)

    def lay(acc, n, plane, col):
        shifted = wide(plane, col)
        zq[tiles - 1] = shifted[:, :LANES]
        zq[tiles] = shifted[:, LANES:]
        begin = tiles - 1 - col // LANES
        for t in range(tiles):
            acc[n, t] = acc[n, t] + zq[begin + t]

    def edge(n, j, beside):
        if beside:
            return behinds[n][0, j] - behind * band, behinds[n][1, j]
        return places[n][0, j] - me * band, places[n][1, j]

    for copy in relay:
        copy.wait()
    twice[0, :patch] = power
    twice[0, patch:] = power
    for n in range(n_ang):
        for beside in (False, True):
            for j in range(count):
                row, col = edge(n, j, beside)
                begin = lax.rem(me_a * ns + 2 * band - jnp.clip(row, -band, band), band)
                lay(lw, n, twice[0, pl.ds(begin, ns), :] * mark(row, beside), col)
    lw[...] = 1.0 / lw[...]

    for j in range(count):
        place_own(acci, whole_patch(j, 1), j)

    def pass_on(g, n):
        outward[g][n].wait()
        copy = remote(rx.at[n, pl.ds(g * size, size)], nrx.at[n + 1, pl.ds(g * size, size)],
                      f_send.at[n + 1, g], f_recv.at[n + 1, g], "pos", ahead)
        copy.start()
        forward[g].append(copy)

    for n in range(n_ang - 1):
        pass_on(0, n)
    for copy in second[-1][1]:
        copy.start()
    for j in range(count):
        place_own(accr, whole_patch(j, 0), j)
    for copy in scatter:
        copy.wait()
    part = numden[:, pl.ds(pl.multiple_of(me * pr, 8), pr), :]
    for d in range(n_pos - 1):
        part = part + rs[d]
    partial[...] = part
    ag[me_a] = part
    gather = [remote(partial, ag.at[me_a], ag_send.at[n], ag_recv.at[n], "angle", peer)
              for n, peer in enumerate(angle_peers)]
    for copy in gather:
        copy.start()

    def project(k, a, lines):
        high, low = halves(lines)
        both = mm(jnp.concatenate([high, low], axis=0), rh[...])
        lines = (both[:ns] + both[ns:] + mm(high, rl[...])) * (math.pi / n_ang)
        high, low = halves(lines)
        next_high, next_low = halves(pltpu.roll(lines, width - 1, 1))
        stack = jnp.concatenate([high, low, next_high, next_low], axis=0)
        for n in range(per_angle):
            z, part = n // per_row, n % per_row
            got = mm(stack, tables[k * per_angle + n])
            lower = got[:ns] + got[ns:2 * ns]
            upper = got[2 * ns:3 * ns] + got[3 * ns:]
            w = weight[pl.ds(a, 1), z, pl.ds(part * chunk, chunk)]
            value = (1.0 - w) * lower + w * upper
            lanes = pl.ds(n * chunk, chunk)
            recon[:, lanes] = value if k == 0 else recon[:, lanes] + value

    def lines_of(n):
        for g, group in enumerate(groups):
            forward[g][n].wait()
            for j in group:
                row, col = edge(n, j, False)
                own = blk[j, pl.ds(pl.multiple_of(me_a * ns, 8), ns), :] if n == 0 else rx[n - 1, j]
                lay(lg, n, own * mark(row, False), col)
                row, col = edge(n, j, True)
                lay(lg, n, nrx[n, j] * mark(row, True), col)
        rows = pl.ds(pl.multiple_of(me_a * ns, 8), ns)
        if n > 0:
            early[n - 1].wait()
        parts = []
        for t in range(tiles):
            base = obj[1, t, rows, :] if n == 0 else orx[n - 1, t]
            parts.append(base + lg[n, t] * lw[n, t])
        project(n, origins[n], jnp.concatenate(parts, axis=1))

    pass_on(1, 0) if len(groups) > 1 else None
    lines_of(0)
    for g in range(1, len(groups)):
        for n in range(1 if g == 1 else 0, n_ang - 1):
            pass_on(g, n)
    for g, group in enumerate(groups):
        for copy in second[g][0]:
            copy.wait()
        for j in group:
            place_above(acci, from_above[j, 1], j)
            place_below(acci, from_below[j, 1], j)
    for t in range(tiles):
        lanes = slice(t * LANES, (t + 1) * LANES)
        newobj[0, 1, :, lanes] = obj[1, t] + acci[t] * accw[t]
    for copy in gather:
        copy.wait()
    total = ag[0]
    for a in range(1, n_ang):
        total = total + ag[a]
    mine = pl.ds(pl.multiple_of(me * pr, 8), pr)
    for c in range(2):
        value = total[c] / (total[2] + 1.0)
        piece[c] = value
        change[c, mine, :] = value
    spread = [
        remote(piece, change.at[:, mine, :], fin_send.at[d], fin_recv.at[d], "pos", peer)
        for d, peer in enumerate(pos_peers)
    ]
    for copy in spread:
        copy.start()
    lines_of(1)
    for g, group in enumerate(groups):
        for copy in second[g][1]:
            copy.wait()
        for j in group:
            place_above(accr, from_above[j, 0], j)
            place_below(accr, from_below[j, 0], j)
    for t in range(tiles):
        lanes = slice(t * LANES, (t + 1) * LANES)
        newobj[0, 0, :, lanes] = obj[0, t] + accr[t] * accw[t]
    for n in range(2, n_ang):
        lines_of(n)
    for copy in spread:
        copy.wait()


def tail_kernel(newobj, recon, change, probe, out_obj, out_probe, out_recon, sem):
    copy = pltpu.make_async_copy(newobj, out_obj, sem.at[0])
    copy.start()
    out_probe[...] = probe[...] + change[...]
    width = out_recon.shape[3]
    for s in range(out_recon.shape[1]):
        for z in range(out_recon.shape[2]):
            out_recon[0, s, z:z + 1, :] = recon[s:s + 1, z * width:(z + 1) * width]
    copy.wait()


def on_device(n_ang, n_pos, amplitude, offsets, probe_field, object_field, interp_index, interp_weight):
    band = object_field.shape[2]
    width = object_field.shape[3]
    patch = probe_field.shape[1]
    half = patch // 2
    count = offsets.shape[1]
    tiles = width // LANES
    f32, i32, bf16 = jnp.float32, jnp.int32, jnp.bfloat16
    n_z = interp_index.shape[1]
    chunk = min(512, width)
    tables = n_ang * n_z * (width // chunk)
    size = 2 if count % 2 == 0 else count
    left, right = dft_blocks(patch)
    ah, al = split_const(left)
    bh, bl = split_const(right)
    vmem = pl.BlockSpec(memory_space=VMEM)
    hbm = pl.BlockSpec(memory_space=pl.ANY)
    sds = jax.ShapeDtypeStruct
    dma = pltpu.SemaphoreType.DMA
    total = n_z * width
    ns = band // n_ang
    pr = patch // n_pos
    lead = max(0, band - half)
    ext = 2 * tiles
    table = VMEM((2 * patch, 2 * patch), bf16)
    half_shape = (count, 2, half, patch)
    bits = (n_ang - 1).bit_length()
    links = 2 + 6 * (count // size)
    base = [
        VMEM((2, tiles, band, LANES), f32), VMEM(amplitude.shape, f32), VMEM(probe_field.shape, f32),
        VMEM(interp_index.shape, i32), VMEM(interp_weight.shape, f32), table, table, table, table,
        [VMEM((size, 2, band + patch, patch), f32)] * (count // size), VMEM((2,) + half_shape, f32),
        VMEM((ext, lead + half + band, LANES), f32),
        VMEM((ext, half + band, LANES), f32), VMEM((ext, half + band, LANES), f32),
    ]
    sums = [
        VMEM((tiles, band, LANES), f32), VMEM((tiles, band, LANES), f32), VMEM((tiles, band, LANES), f32),
        VMEM((2,) + half_shape, f32), VMEM(half_shape, f32), VMEM(half_shape, f32),
    ]
    parts = [VMEM((3, patch, patch), f32), VMEM((n_pos - 1, 3, pr, patch), f32)]
    filters = [VMEM((tables, width, chunk), bf16), VMEM((width, width), bf16), VMEM((width, width), bf16)]
    groups, peers = count // size, n_ang - 1
    sems = [dma((9 + tiles,)), dma((links,)), dma((links,)), dma((n_pos - 1,)), dma((n_pos - 1,))]
    ends = [dma((n_pos - 1,)), dma((n_pos - 1,))]
    lines = VMEM((n_ang, tiles, ns, LANES), f32)
    offsets_of = pltpu.SMEM((2, count), i32)
    if band == patch:
        kernel = slice_kernel
        scratch = [
            offsets_of, pltpu.SMEM((2, 2, count), i32), pltpu.SMEM((peers, 2, count), i32),
            pltpu.SMEM((peers, 2, count), i32), *base, VMEM((ext, ns, LANES), f32), *sums,
            VMEM((size, 2 * patch, patch), f32), VMEM((count, band, patch), f32),
            VMEM((peers, tiles, ns, LANES), f32), VMEM((peers, count, ns, LANES), f32),
            VMEM((n_ang, count, ns, LANES), f32), lines, lines, *parts,
            VMEM((3, pr, patch), f32), VMEM((n_ang, 3, pr, patch), f32), VMEM((2, pr, patch), f32), *filters,
            *sems, dma((peers,)), dma((peers,)), dma((peers,)), dma((peers,)), dma((peers,)), dma((peers,)),
            dma((peers, groups)), dma((peers, groups)), dma((n_ang, groups)), dma((n_ang, groups)),
            dma((peers,)), dma((peers,)), *ends,
        ]
    else:
        kernel = step_kernel
        scratch = [
            offsets_of, pltpu.SMEM((2, 2, count), i32), *base, *sums, *parts,
            VMEM((bits, 3, pr, patch), f32), VMEM((bits, 3, pr, patch), f32), VMEM((2, pr, patch), f32),
            VMEM((peers, ns, width), f32), *filters, *sems,
            dma((peers,)), dma((peers,)), dma((bits,)), dma((bits,)), *ends,
        ]
    newobj, recon, change = pl.pallas_call(
        functools.partial(kernel, n_ang, n_pos, size),
        out_shape=(VMEM(object_field.shape, f32), VMEM((ns, total), f32), VMEM(probe_field.shape, f32)),
        in_specs=[hbm] * 10,
        out_specs=(vmem,) * 3,
        scratch_shapes=scratch,
        compiler_params=pltpu.CompilerParams(
            collective_id=0, has_side_effects=True, vmem_limit_bytes=KLIMIT),
        name="step",
    )(*(pltpu.with_memory_space_constraint(x, pltpu.HBM) for x in (
        jnp.transpose(offsets[0]), object_field, amplitude, probe_field, interp_index, interp_weight,
        ah, al, bh, bl)))
    out = pl.pallas_call(
        tail_kernel,
        out_shape=(sds(object_field.shape, f32), sds(probe_field.shape, f32), sds((1, ns, n_z, width), f32)),
        in_specs=[vmem] * 4,
        out_specs=(hbm, vmem, vmem),
        scratch_shapes=[dma((1,))],
        compiler_params=pltpu.CompilerParams(vmem_limit_bytes=TLIMIT),
        name="tail",
    )(newobj, recon, change, probe_field)
    return tuple(out)


KLIMIT = 48 * 1024 * 1024
TLIMIT = 8 * 1024 * 1024


def solution(mesh):
    placed = (
        P("angle", "pos", None, None),
        P("angle", "pos", None),
        P(),
        P("angle", None, "pos", None),
        P(),
        P(),
    )
    return jax.shard_map(
        functools.partial(on_device, mesh.shape["angle"], mesh.shape["pos"]),
        mesh=mesh,
        in_specs=placed,
        out_specs=(P("angle", None, "pos", None), P(), P("pos", "angle", None, None)),
        check_vma=False,
    )
```

```python
import functools
import math

import jax
import jax.numpy as jnp
import numpy as np
from jax import lax
from jax.experimental import pallas as pl
from jax.experimental.pallas import tpu as pltpu
from jax.sharding import PartitionSpec as P

MESH = pl.DeviceIdType.MESH
VMEM = pltpu.VMEM
LANES = 128


def split_const(table):
    high = jnp.asarray(table, jnp.float32).astype(jnp.bfloat16)
    low = (jnp.asarray(table, jnp.float32) - high.astype(jnp.float32)).astype(jnp.bfloat16)
    return high, low


def dft_blocks(length):
    ramp = np.arange(length)
    theta = (ramp[:, None] * ramp[None, :] % length) * (2.0 * math.pi / length)
    real = np.cos(theta) / math.sqrt(length)
    imag = -np.sin(theta) / math.sqrt(length)
    left = np.block([[real, -imag], [imag, real]])
    right = np.block([[real, imag], [-imag, real]])
    return np.asarray(left, np.float32), np.asarray(right, np.float32)


def halves(value):
    high = value.astype(jnp.bfloat16)
    return high, (value - high.astype(jnp.float32)).astype(jnp.bfloat16)


def mm(a, b):
    return jnp.dot(a, b, preferred_element_type=jnp.float32)


def left3(table_high, table_low, value):
    high, low = halves(value)
    return mm(table_high, high) + mm(table_high, low) + mm(table_low, high)


def right3(value, table_high, table_low):
    high, low = halves(value)
    return mm(high, table_high) + mm(low, table_high) + mm(high, table_low)


def remote(src, dst, send, recv, axis, target):
    return pltpu.make_async_remote_copy(
        src_ref=src, dst_ref=dst, send_sem=send, recv_sem=recv,
        device_id={axis: target}, device_id_type=MESH,
    )


def flip(me, mask, bits):
    other = 0
    for b in range(bits):
        bit = (me // (1 << b)) % 2
        other = other + (1 << b) * (1 - bit if (mask >> b) & 1 else bit)
    return other


def step_kernel(n_ang, n_pos, size,
                offs_h, obj_h, amp_h, probe_h, index_h, weight_h, ah_h, al_h, bh_h, bl_h,
                newobj, recon, change,
                offs, near, obj, amp, probe, index, weight, ah, al, bh, bl,
                ext, sb, zo, za, zb, accw, acci, accr, grad, from_above, from_below,
                numden, rs, partial, ag, piece, sino, tables, rh, rl,
                in_sem, send_sem, recv_sem, rs_send, rs_recv,
                a2a_send, a2a_recv, ag_send, ag_recv, fin_send, fin_recv):
    me_a = lax.axis_index("angle")
    me = lax.axis_index("pos")
    up, down = lax.rem(me + n_pos - 1, n_pos), lax.rem(me + 1, n_pos)
    tiles, band = obj.shape[1], obj.shape[2]
    width = tiles * LANES
    patch = probe.shape[1]
    half = patch // 2
    count = amp.shape[1]
    ns = sino.shape[1]

    sources = [(offs_h, offs), (probe_h, probe), (amp_h, amp),
               (ah_h, ah), (al_h, al), (bh_h, bh), (bl_h, bl), (index_h, index), (weight_h, weight)]
    sources += [(obj_h.at[0, :, :, pl.ds(t * LANES, LANES)], obj.at[:, t]) for t in range(tiles)]
    loads = [pltpu.make_async_copy(src, dst, in_sem.at[k]) for k, (src, dst) in enumerate(sources)]
    for copy in loads:
        copy.start()
    bits = (n_ang - 1).bit_length()
    order = [1] + list(range(n_ang - 1, 1, -1))
    angle_peers = [flip(me_a, mask, bits) for mask in order]
    pos_peers = [lax.rem(me + d, n_pos) for d in range(1, n_pos)]
    barrier = pltpu.get_barrier_semaphore()
    for peer in pos_peers:
        pl.semaphore_signal(barrier, inc=1, device_id={"pos": peer}, device_id_type=MESH)
    for peer in angle_peers:
        pl.semaphore_signal(barrier, inc=1, device_id={"angle": peer}, device_id_type=MESH)
    loads[0].wait()
    pl.semaphore_wait(barrier, n_ang + n_pos - 2)
    swap = [remote(offs, near.at[0], send_sem.at[0], recv_sem.at[0], "pos", down),
            remote(offs, near.at[1], send_sem.at[1], recv_sem.at[1], "pos", up)]
    for copy in swap:
        copy.start()
    for copy in loads[9:]:
        copy.wait()

    def columns(c, rows, col):
        tile = col // LANES
        after = jnp.minimum(tile + 1, tiles - 1)
        got = jnp.concatenate([obj[c, tile, rows, :], obj[c, after, rows, :]], axis=1)
        return pltpu.roll(got, lax.rem(2 * LANES - lax.rem(col, LANES), 2 * LANES), 1)[:, :patch]

    for j in range(count):
        for c in range(2):
            ext[j // size][j % size, c, half:half + band, :] = columns(c, slice(0, band), offs[1, j])
    zo[...] = jnp.zeros_like(zo)
    za[...] = jnp.zeros_like(za)
    zb[...] = jnp.zeros_like(zb)
    for k, copy in enumerate(swap):
        copy.wait()
    first = []
    groups = [range(g * size, (g + 1) * size) for g in range(count // size)]
    for g, group in enumerate(groups):
        for j in group:
            for c in range(2):
                sb[0, j, c] = columns(c, slice(band - half, band), near[1, 1, j])
                sb[1, j, c] = columns(c, slice(0, half), near[0, 1, j])
        span = pl.ds(g * size, size)
        pair = [
            remote(sb.at[0, span], ext[g].at[:, :, pl.ds(0, half), :],
                   send_sem.at[2 + 6 * g], recv_sem.at[2 + 6 * g], "pos", down),
            remote(sb.at[1, span], ext[g].at[:, :, pl.ds(half + band, half), :],
                   send_sem.at[3 + 6 * g], recv_sem.at[3 + 6 * g], "pos", up),
        ]
        for copy in pair:
            copy.start()
        first.append(pair)

    def spot(row, col, owner):
        return jnp.clip(row - owner * band + half, 0, band), col

    own_at = [spot(offs[0, j], offs[1, j], me) for j in range(count)]
    above_at = [spot(near[0, 0, j], near[0, 1, j], up) for j in range(count)]
    below_at = [spot(near[1, 0, j], near[1, 1, j], down) for j in range(count)]

    def wide(plane, col):
        blank = jnp.zeros((plane.shape[0], LANES), jnp.float32)
        both = jnp.concatenate([plane, blank], axis=1)
        return pltpu.roll(both, lax.rem(col, LANES), 1)

    lead = max(0, band - half)

    def place(acc, buf, first_row, plane, start, rows, col):
        shifted = wide(plane, col)
        where = slice(first_row, first_row + plane.shape[0])
        buf[tiles - 1, where, :] = shifted[:, :LANES]
        buf[tiles, where, :] = shifted[:, LANES:]
        begin = tiles - 1 - col // LANES
        for t in range(tiles):
            acc[t, rows, :] = acc[t, rows, :] + buf[begin + t, pl.ds(start, rows.stop - rows.start), :]

    def place_own(acc, plane, j):
        row, col = own_at[j]
        place(acc, zo, lead, plane, lead + half - row, slice(0, band), col)

    def place_above(acc, plane, j):
        row, col = above_at[j]
        place(acc, za, 0, plane, band - row, slice(0, half), col)

    def place_below(acc, plane, j):
        row, col = below_at[j]
        place(acc, zb, band, plane, band - row, slice(band - half, band), col)

    loads[1].wait()
    p_re, p_im = probe[0], probe[1]
    power = p_re * p_re + p_im * p_im
    accw[...] = jnp.ones_like(accw)
    acci[...] = jnp.zeros_like(acci)
    accr[...] = jnp.zeros_like(accr)
    for j in range(count):
        place_own(accw, power, j)
        place_above(accw, power[half:], j)
        place_below(accw, power[:half], j)
    accw[...] = 1.0 / accw[...]
    tall = 64

    def ramp(step, carry):
        top = pl.multiple_of(step * tall, tall)
        shape = (tall, width)
        differ = lax.broadcasted_iota(jnp.int32, shape, 1) - (
            lax.broadcasted_iota(jnp.int32, shape, 0) + top)
        spread = differ.astype(jnp.float32)
        odd = -1.0 / (jnp.maximum(spread * spread, 1.0) * (math.pi * math.pi))
        value = jnp.where((differ & 1) == 1, odd, jnp.where(differ == 0, 0.25, 0.0))
        rh[pl.ds(top, tall), :], rl[pl.ds(top, tall), :] = halves(value)
        return carry

    lax.fori_loop(0, width // tall, ramp, 0)
    for copy in loads[2:9]:
        copy.wait()
    chunk = tables.shape[2]
    per_row = width // chunk
    zwin = index.shape[1]
    per_angle = zwin * per_row
    deep = 16
    pattern = lax.broadcasted_iota(jnp.int32, (deep, chunk), 0)
    one, zero = jnp.ones((deep, chunk), jnp.bfloat16), jnp.zeros((deep, chunk), jnp.bfloat16)
    pattern = pattern.astype(jnp.int16)

    origins = [me_a] + angle_peers

    def build(k, step, carry):
        a = origins[k]
        z = step // per_row
        lanes = pl.ds(pl.multiple_of(lax.rem(step, per_row) * chunk, chunk), chunk)
        at = jnp.broadcast_to(index[a, pl.ds(z, 1), lanes], (deep, chunk)).astype(jnp.int16)
        for r in range(width // deep):
            hit = at == pattern + jnp.int16(r * deep)
            tables[k * per_angle + step, r * deep:(r + 1) * deep, :] = jnp.where(hit, one, zero)
        return carry

    def build_all(k):
        lax.fori_loop(0, per_angle, functools.partial(build, k), 0)

    for k in range(n_ang):
        build_all(k)
    n_re = jnp.zeros((patch, patch), jnp.float32)
    n_im = n_re
    den = n_re
    second = []
    for g, group in enumerate(groups):
        for copy in first[g]:
            copy.wait()
        q_re, q_im, w_re, w_im = [], [], [], []
        for j in group:
            rows = pl.ds(own_at[j][0], patch)
            re, im = ext[g][j % size, 0, rows, :], ext[g][j % size, 1, rows, :]
            q_re.append(re)
            q_im.append(im)
            w_re.append(p_re * re - p_im * im)
            w_im.append(p_re * im + p_im * re)
        psi = jnp.concatenate([jnp.concatenate(w_re, axis=1), jnp.concatenate(w_im, axis=1)], axis=0)
        mid = left3(ah[...], al[...], psi)
        cells = [slice(n * patch, (n + 1) * patch) for n in range(size)]
        rows = [jnp.concatenate([mid[:patch, cell], mid[patch:, cell]], axis=1) for cell in cells]
        spec = right3(jnp.concatenate(rows, axis=0), bh[...], bl[...])
        fixed = []
        for j, cell in zip(group, cells):
            s_re = spec[cell, :patch]
            s_im = spec[cell, patch:]
            factor = amp[0, j] / jnp.maximum(jnp.sqrt(s_re * s_re + s_im * s_im), 0.5)
            fixed.append(jnp.concatenate([factor * s_re, factor * s_im], axis=1))
        back = right3(jnp.concatenate(fixed, axis=0), ah[...], al[...])
        wide_re = jnp.concatenate([back[cell, :patch] for cell in cells], axis=1)
        wide_im = jnp.concatenate([back[cell, patch:] for cell in cells], axis=1)
        diff = left3(bh[...], bl[...], jnp.concatenate([wide_re, wide_im], axis=0))
        diff = diff - psi
        for n, j in enumerate(group):
            d_re, d_im = diff[:patch, cells[n]], diff[patch:, cells[n]]
            g_re = p_re * d_re + p_im * d_im
            g_im = p_re * d_im - p_im * d_re
            for h in range(2):
                grad[h, j, 0] = g_re[h * half:(h + 1) * half]
                grad[h, j, 1] = g_im[h * half:(h + 1) * half]
            n_re = n_re + (q_re[n] * d_re + q_im[n] * d_im)
            n_im = n_im + (q_re[n] * d_im - q_im[n] * d_re)
            den = den + (q_re[n] * q_re[n] + q_im[n] * q_im[n])
        span = pl.ds(g * size, size)
        pairs = []
        for c in (1, 0):
            k = 4 + 6 * g + 2 * (1 - c)
            pairs.append([
                remote(grad.at[1, span, c], from_above.at[span, c], send_sem.at[k], recv_sem.at[k], "pos", down),
                remote(grad.at[0, span, c], from_below.at[span, c], send_sem.at[k + 1], recv_sem.at[k + 1], "pos", up),
            ])
        for copy in pairs[0] + ([] if g == len(groups) - 1 else pairs[1]):
            copy.start()
        second.append(pairs)
    numden[0] = n_re
    numden[1] = n_im
    numden[2] = den
    pr = patch // n_pos
    scatter = [
        remote(numden.at[:, pl.ds(pl.multiple_of(peer * pr, 8), pr), :], rs.at[d],
               rs_send.at[d], rs_recv.at[d], "pos", peer)
        for d, peer in enumerate(pos_peers)
    ]
    for copy in scatter + second[-1][1]:
        copy.start()

    def whole_patch(j, c):
        return jnp.concatenate([grad[0, j, c], grad[1, j, c]], axis=0)

    for j in range(count):
        place_own(acci, whole_patch(j, 1), j)
    for g, group in enumerate(groups):
        for copy in second[g][0]:
            copy.wait()
        for j in group:
            place_above(acci, from_above[j, 1], j)
            place_below(acci, from_below[j, 1], j)
    for t in range(tiles):
        lanes = slice(t * LANES, (t + 1) * LANES)
        newobj[0, 1, :, lanes] = obj[1, t] + acci[t] * accw[t]
    def project(k, a, lines):
        high, low = halves(lines)
        both = mm(jnp.concatenate([high, low], axis=0), rh[...])
        lines = (both[:ns] + both[ns:] + mm(high, rl[...])) * (math.pi / n_ang)
        high, low = halves(lines)
        next_high, next_low = halves(pltpu.roll(lines, width - 1, 1))
        stack = jnp.concatenate([high, low, next_high, next_low], axis=0)
        for n in range(per_angle):
            z, part = n // per_row, n % per_row
            got = mm(stack, tables[k * per_angle + n])
            lower = got[:ns] + got[ns:2 * ns]
            upper = got[2 * ns:3 * ns] + got[3 * ns:]
            w = weight[pl.ds(a, 1), z, pl.ds(part * chunk, chunk)]
            value = (1.0 - w) * lower + w * upper
            lanes = pl.ds(n * chunk, chunk)
            recon[:, lanes] = value if k == 0 else recon[:, lanes] + value

    across = [
        remote(newobj.at[0, 1, pl.ds(pl.multiple_of(peer * ns, 8), ns), :], sino.at[k],
               a2a_send.at[k], a2a_recv.at[k], "angle", peer)
        for k, peer in enumerate(angle_peers)
    ]
    inner = (me_a >= n_ang // 4) & (me_a < n_ang - n_ang // 4)
    across[0].start()

    @pl.when(inner)
    def _():
        for copy in across[1:-1]:
            copy.start()

    for copy in scatter:
        copy.wait()
    part = numden[:, pl.ds(pl.multiple_of(me * pr, 8), pr), :]
    for d in range(n_pos - 1):
        part = part + rs[d]
    partial[0] = part
    shares = [
        remote(partial.at[b], ag.at[b], ag_send.at[b], ag_recv.at[b], "angle", flip(me_a, 1 << b, bits))
        for b in range(bits)
    ]
    shares[0].start()

    @pl.when(jnp.logical_not(inner))
    def _():
        for copy in across[1:-1]:
            copy.start()

    project(0, me_a, newobj[0, 1, pl.ds(pl.multiple_of(me_a * ns, 8), ns), :])
    for b in range(bits - 1):
        shares[b].wait()
        partial[b + 1] = partial[b] + ag[b]
        shares[b + 1].start()
    across[-1].start()
    for g, group in enumerate(groups):
        for copy in second[g][1]:
            copy.wait()
        for j in group:
            place_own(accr, whole_patch(j, 0), j)
            place_above(accr, from_above[j, 0], j)
            place_below(accr, from_below[j, 0], j)
    for t in range(tiles):
        lanes = slice(t * LANES, (t + 1) * LANES)
        newobj[0, 0, :, lanes] = obj[0, t] + accr[t] * accw[t]
    shares[-1].wait()
    total = partial[bits - 1] + ag[bits - 1]
    mine = pl.ds(pl.multiple_of(me * pr, 8), pr)
    for c in range(2):
        value = total[c] / (total[2] + 1.0)
        piece[c] = value
        change[c, mine, :] = value
    spread = [
        remote(piece, change.at[:, mine, :], fin_send.at[d], fin_recv.at[d], "pos", peer)
        for d, peer in enumerate(pos_peers)
    ]
    for copy in spread:
        copy.start()
    for k, peer in enumerate(angle_peers):
        across[k].wait()
        project(k + 1, peer, sino[k])
    for copy in spread:
        copy.wait()


def slice_kernel(n_ang, n_pos, size,
                 offs_h, obj_h, amp_h, probe_h, index_h, weight_h, ah_h, al_h, bh_h, bl_h,
                 newobj, recon, change,
                 offs, near, far, farn, obj, amp, probe, index, weight, ah, al, bh, bl,
                 ext, sb, zo, za, zb, zq, accw, acci, accr, grad, from_above, from_below,
                 twice, blk, orx, rx, nrx, lw, lg,
                 numden, rs, paired, partial, ag, piece, tables, rh, rl,
                 in_sem, send_sem, recv_sem, rs_send, rs_recv, pair_sem, far_send, far_recv, farn_send, farn_recv,
                 o_send, o_recv, z_send, z_recv, f_send, f_recv, ag_send, ag_recv, fin_send, fin_recv):
    me_a = lax.axis_index("angle")
    me = lax.axis_index("pos")
    up, down = lax.rem(me + n_pos - 1, n_pos), lax.rem(me + 1, n_pos)
    tiles, band = obj.shape[1], obj.shape[2]
    width = tiles * LANES
    patch = probe.shape[1]
    half = patch // 2
    count = amp.shape[1]
    ns = orx.shape[2]
    side = (me_a * ns) // half
    ahead = lax.rem(me + n_pos + 1 - 2 * side, n_pos)
    behind = lax.rem(me + n_pos - 1 + 2 * side, n_pos)

    sources = [(offs_h, offs), (probe_h, probe), (amp_h, amp),
               (ah_h, ah), (al_h, al), (bh_h, bh), (bl_h, bl), (index_h, index), (weight_h, weight)]
    sources += [(obj_h.at[0, :, :, pl.ds(t * LANES, LANES)], obj.at[:, t]) for t in range(tiles)]
    loads = [pltpu.make_async_copy(src, dst, in_sem.at[k]) for k, (src, dst) in enumerate(sources)]
    for copy in loads:
        copy.start()
    bits = (n_ang - 1).bit_length()
    order = [1] + list(range(n_ang - 1, 1, -1))
    angle_peers = [flip(me_a, mask, bits) for mask in order]
    pos_peers = [lax.rem(me + d, n_pos) for d in range(1, n_pos)]
    barrier = pltpu.get_barrier_semaphore()
    for peer in pos_peers:
        pl.semaphore_signal(barrier, inc=1, device_id={"pos": peer}, device_id_type=MESH)
    for peer in angle_peers:
        pl.semaphore_signal(barrier, inc=1, device_id={"angle": peer}, device_id_type=MESH)
    loads[0].wait()
    pl.semaphore_wait(barrier, n_ang + n_pos - 2)
    swap = [remote(offs, near.at[0], send_sem.at[0], recv_sem.at[0], "pos", down),
            remote(offs, near.at[1], send_sem.at[1], recv_sem.at[1], "pos", up)]
    reach = [remote(offs, far.at[n], far_send.at[n], far_recv.at[n], "angle", peer)
             for n, peer in enumerate(angle_peers)]
    for copy in swap + reach:
        copy.start()
    for copy in loads[9:]:
        copy.wait()
    early = [remote(obj.at[1, :, pl.ds(pl.multiple_of(peer * ns, 8), ns), :], orx.at[n],
                    o_send.at[n], o_recv.at[n], "angle", peer)
             for n, peer in enumerate(angle_peers)]
    for copy in early:
        copy.start()

    def columns(c, rows, col):
        tile = col // LANES
        after = jnp.minimum(tile + 1, tiles - 1)
        got = jnp.concatenate([obj[c, tile, rows, :], obj[c, after, rows, :]], axis=1)
        return pltpu.roll(got, lax.rem(2 * LANES - lax.rem(col, LANES), 2 * LANES), 1)[:, :patch]

    for j in range(count):
        for c in range(2):
            ext[j // size][j % size, c, half:half + band, :] = columns(c, slice(0, band), offs[1, j])
    zo[...] = jnp.zeros_like(zo)
    za[...] = jnp.zeros_like(za)
    zb[...] = jnp.zeros_like(zb)
    zq[...] = jnp.zeros_like(zq)
    lg[...] = jnp.zeros_like(lg)
    lw[...] = jnp.ones_like(lw)
    for k, copy in enumerate(swap):
        copy.wait()
    relay = [remote(far.at[n], farn.at[n], farn_send.at[n], farn_recv.at[n], "pos", ahead)
             for n in range(n_ang - 1)]
    for n in range(n_ang - 1):
        reach[n].wait()
        relay[n].start()
    first = []
    groups = [range(g * size, (g + 1) * size) for g in range(count // size)]
    for g, group in enumerate(groups):
        for j in group:
            for c in range(2):
                sb[0, j, c] = columns(c, slice(band - half, band), near[1, 1, j])
                sb[1, j, c] = columns(c, slice(0, half), near[0, 1, j])
        span = pl.ds(g * size, size)
        pair = [
            remote(sb.at[0, span], ext[g].at[:, :, pl.ds(0, half), :],
                   send_sem.at[2 + 6 * g], recv_sem.at[2 + 6 * g], "pos", down),
            remote(sb.at[1, span], ext[g].at[:, :, pl.ds(half + band, half), :],
                   send_sem.at[3 + 6 * g], recv_sem.at[3 + 6 * g], "pos", up),
        ]
        for copy in pair:
            copy.start()
        first.append(pair)

    def spot(row, col, owner):
        return jnp.clip(row - owner * band + half, 0, band), col

    own_at = [spot(offs[0, j], offs[1, j], me) for j in range(count)]
    above_at = [spot(near[0, 0, j], near[0, 1, j], up) for j in range(count)]
    below_at = [spot(near[1, 0, j], near[1, 1, j], down) for j in range(count)]

    def wide(plane, col):
        blank = jnp.zeros((plane.shape[0], LANES), jnp.float32)
        both = jnp.concatenate([plane, blank], axis=1)
        return pltpu.roll(both, lax.rem(col, LANES), 1)

    lead = max(0, band - half)

    def place(acc, buf, first_row, plane, start, rows, col):
        shifted = wide(plane, col)
        where = slice(first_row, first_row + plane.shape[0])
        buf[tiles - 1, where, :] = shifted[:, :LANES]
        buf[tiles, where, :] = shifted[:, LANES:]
        begin = tiles - 1 - col // LANES
        for t in range(tiles):
            acc[t, rows, :] = acc[t, rows, :] + buf[begin + t, pl.ds(start, rows.stop - rows.start), :]

    def place_own(acc, plane, j):
        row, col = own_at[j]
        place(acc, zo, lead, plane, lead + half - row, slice(0, band), col)

    def place_above(acc, plane, j):
        row, col = above_at[j]
        place(acc, za, 0, plane, band - row, slice(0, half), col)

    def place_below(acc, plane, j):
        row, col = below_at[j]
        place(acc, zb, band, plane, band - row, slice(band - half, band), col)

    loads[1].wait()
    p_re, p_im = probe[0], probe[1]
    power = p_re * p_re + p_im * p_im
    accw[...] = jnp.ones_like(accw)
    acci[...] = jnp.zeros_like(acci)
    accr[...] = jnp.zeros_like(accr)
    for j in range(count):
        place_own(accw, power, j)
        place_above(accw, power[half:], j)
        place_below(accw, power[:half], j)
    accw[...] = 1.0 / accw[...]
    tall = 64

    def ramp(step, carry):
        top = pl.multiple_of(step * tall, tall)
        shape = (tall, width)
        differ = lax.broadcasted_iota(jnp.int32, shape, 1) - (
            lax.broadcasted_iota(jnp.int32, shape, 0) + top)
        spread = differ.astype(jnp.float32)
        odd = -1.0 / (jnp.maximum(spread * spread, 1.0) * (math.pi * math.pi))
        value = jnp.where((differ & 1) == 1, odd, jnp.where(differ == 0, 0.25, 0.0))
        rh[pl.ds(top, tall), :], rl[pl.ds(top, tall), :] = halves(value)
        return carry

    lax.fori_loop(0, width // tall, ramp, 0)
    for copy in loads[2:9]:
        copy.wait()
    chunk = tables.shape[2]
    per_row = width // chunk
    zwin = index.shape[1]
    per_angle = zwin * per_row
    deep = 16
    pattern = lax.broadcasted_iota(jnp.int32, (deep, chunk), 0)
    one, zero = jnp.ones((deep, chunk), jnp.bfloat16), jnp.zeros((deep, chunk), jnp.bfloat16)
    pattern = pattern.astype(jnp.int16)

    origins = [me_a] + angle_peers

    def build(k, step, carry):
        a = origins[k]
        z = step // per_row
        lanes = pl.ds(pl.multiple_of(lax.rem(step, per_row) * chunk, chunk), chunk)
        at = jnp.broadcast_to(index[a, pl.ds(z, 1), lanes], (deep, chunk)).astype(jnp.int16)
        for r in range(width // deep):
            hit = at == pattern + jnp.int16(r * deep)
            tables[k * per_angle + step, r * deep:(r + 1) * deep, :] = jnp.where(hit, one, zero)
        return carry

    def build_all(k):
        lax.fori_loop(0, per_angle, functools.partial(build, k), 0)

    for k in range(n_ang):
        build_all(k)
    places = [offs] + [far.at[n] for n in range(n_ang - 1)]
    behinds = [near.at[side]] + [farn.at[n] for n in range(n_ang - 1)]
    slot = lax.broadcasted_iota(jnp.int32, (ns, LANES), 0) + me_a * ns

    def mark(row, beside):
        if beside:
            return jnp.where(side == 0, (slot < row).astype(jnp.float32), (slot >= row + band).astype(jnp.float32))
        return ((slot >= row) & (slot < row + band)).astype(jnp.float32)

    def lay(acc, n, plane, col):
        shifted = wide(plane, col)
        zq[tiles - 1] = shifted[:, :LANES]
        zq[tiles] = shifted[:, LANES:]
        begin = tiles - 1 - col // LANES
        for t in range(tiles):
            acc[n, t] = acc[n, t] + zq[begin + t]

    def edge(n, j, beside):
        if beside:
            return behinds[n][0, j] - behind * band, behinds[n][1, j]
        return places[n][0, j] - me * band, places[n][1, j]

    for copy in relay:
        copy.wait()
    twice[0, :patch] = power
    twice[0, patch:] = power
    for n in range(n_ang):
        for beside in (False, True):
            for j in range(count):
                row, col = edge(n, j, beside)
                begin = lax.rem(me_a * ns + 2 * band - jnp.clip(row, -band, band), band)
                lay(lw, n, twice[0, pl.ds(begin, ns), :] * mark(row, beside), col)
    lw[...] = 1.0 / lw[...]

    n_re = jnp.zeros((patch, patch), jnp.float32)
    n_im = n_re
    den = n_re
    second, outward, forward = [], [], []
    for g, group in enumerate(groups):
        for copy in first[g]:
            copy.wait()
        q_re, q_im, w_re, w_im = [], [], [], []
        for j in group:
            rows = pl.ds(own_at[j][0], patch)
            re, im = ext[g][j % size, 0, rows, :], ext[g][j % size, 1, rows, :]
            q_re.append(re)
            q_im.append(im)
            w_re.append(p_re * re - p_im * im)
            w_im.append(p_re * im + p_im * re)
        psi = jnp.concatenate([jnp.concatenate(w_re, axis=1), jnp.concatenate(w_im, axis=1)], axis=0)
        mid = left3(ah[...], al[...], psi)
        cells = [slice(n * patch, (n + 1) * patch) for n in range(size)]
        rows = [jnp.concatenate([mid[:patch, cell], mid[patch:, cell]], axis=1) for cell in cells]
        spec = right3(jnp.concatenate(rows, axis=0), bh[...], bl[...])
        fixed = []
        for j, cell in zip(group, cells):
            s_re = spec[cell, :patch]
            s_im = spec[cell, patch:]
            factor = amp[0, j] / jnp.maximum(jnp.sqrt(s_re * s_re + s_im * s_im), 0.5)
            fixed.append(jnp.concatenate([factor * s_re, factor * s_im], axis=1))
        back = right3(jnp.concatenate(fixed, axis=0), ah[...], al[...])
        wide_re = jnp.concatenate([back[cell, :patch] for cell in cells], axis=1)
        wide_im = jnp.concatenate([back[cell, patch:] for cell in cells], axis=1)
        diff = left3(bh[...], bl[...], jnp.concatenate([wide_re, wide_im], axis=0))
        diff = diff - psi
        for n, j in enumerate(group):
            d_re, d_im = diff[:patch, cells[n]], diff[patch:, cells[n]]
            g_re = p_re * d_re + p_im * d_im
            g_im = p_re * d_im - p_im * d_re
            twice[n, :patch] = g_im
            twice[n, patch:] = g_im
            blk[j] = twice[n, pl.ds(lax.rem(2 * band - (offs[0, j] - me * band), band), band), :]
            for h in range(2):
                grad[h, j, 0] = g_re[h * half:(h + 1) * half]
                grad[h, j, 1] = g_im[h * half:(h + 1) * half]
            n_re = n_re + (q_re[n] * d_re + q_im[n] * d_im)
            n_im = n_im + (q_re[n] * d_im - q_im[n] * d_re)
            den = den + (q_re[n] * q_re[n] + q_im[n] * q_im[n])
        span = pl.ds(g * size, size)
        out = [remote(blk.at[span, pl.ds(pl.multiple_of(peer * ns, 8), ns), :], rx.at[n, span],
                      z_send.at[n, g], z_recv.at[n, g], "angle", peer)
               for n, peer in enumerate(angle_peers)]
        mine = remote(blk.at[span, pl.ds(pl.multiple_of(me_a * ns, 8), ns), :], nrx.at[0, span],
                      f_send.at[0, g], f_recv.at[0, g], "pos", ahead)
        for copy in out + [mine]:
            copy.start()
        outward.append(out)
        forward.append([mine])
        pairs = []
        for c in (1, 0):
            k = 4 + 6 * g + 2 * (1 - c)
            pairs.append([
                remote(grad.at[1, span, c], from_above.at[span, c], send_sem.at[k], recv_sem.at[k], "pos", down),
                remote(grad.at[0, span, c], from_below.at[span, c], send_sem.at[k + 1], recv_sem.at[k + 1], "pos", up),
            ])
        for copy in pairs[0] + ([] if g == len(groups) - 1 else pairs[1]):
            copy.start()
        second.append(pairs)
    numden[0] = n_re
    numden[1] = n_im
    numden[2] = den
    pr = patch // n_pos
    core, chip, chips = me % 2, me // 2, n_pos // 2
    swap_half = remote(numden.at[:, pl.ds(pl.multiple_of((1 - core) * half, 8), half), :], paired.at[0],
                       pair_sem.at[0], pair_sem.at[1], "pos", me + 1 - 2 * core)
    swap_half.start()

    def whole_patch(j, c):
        return jnp.concatenate([grad[0, j, c], grad[1, j, c]], axis=0)

    for j in range(count):
        place_own(acci, whole_patch(j, 1), j)
    swap_half.wait()
    paired[1] = paired[0] + numden[:, pl.ds(pl.multiple_of(core * half, 8), half), :]
    chip_peers = [lax.rem(chip + d, chips) for d in range(1, chips)]
    scatter = [
        remote(paired.at[1, :, pl.ds(pl.multiple_of(peer * pr, 8), pr), :], rs.at[d],
               rs_send.at[d], rs_recv.at[d], "pos", 2 * peer + core)
        for d, peer in enumerate(chip_peers)
    ]
    for copy in scatter:
        copy.start()

    def pass_on(g, n):
        outward[g][n].wait()
        copy = remote(rx.at[n, pl.ds(g * size, size)], nrx.at[n + 1, pl.ds(g * size, size)],
                      f_send.at[n + 1, g], f_recv.at[n + 1, g], "pos", ahead)
        copy.start()
        forward[g].append(copy)

    gather = [remote(partial, ag.at[me_a], ag_send.at[n], ag_recv.at[n], "angle", peer)
              for n, peer in enumerate(angle_peers)]

    def share():
        for copy in scatter:
            copy.wait()
        part = paired[1, :, pl.ds(pl.multiple_of(chip * pr, 8), pr), :]
        for d in range(chips - 1):
            part = part + rs[d]
        partial[...] = part
        ag[me_a] = part
        for copy in gather:
            copy.start()

    origins_of = [me_a] + angle_peers
    here = pl.ds(pl.multiple_of(me_a * ns, 8), ns)

    def lay_own(g, n):
        for j in groups[g]:
            row, col = edge(n, j, False)
            own = blk[j, here, :] if n == 0 else rx[n - 1, j]
            lay(lg, n, own * mark(row, False), col)

    def lay_beside(g, n):
        forward[g][n].wait()
        for j in groups[g]:
            row, col = edge(n, j, True)
            lay(lg, n, nrx[n, j] * mark(row, True), col)

    def filtered(ns_of):
        tops, lows = [], []
        for n in ns_of:
            parts = []
            for t in range(tiles):
                base = obj[1, t, here, :] if n == 0 else orx[n - 1, t]
                parts.append(base + lg[n, t] * lw[n, t])
            high, low = halves(jnp.concatenate(parts, axis=1))
            tops.append(high)
            lows.append(low)
        both = mm(jnp.concatenate(tops + lows, axis=0), rh[...])
        more = mm(jnp.concatenate(tops, axis=0), rl[...])
        size_of = len(ns_of) * ns
        total = (both[:size_of] + both[size_of:] + more) * (math.pi / n_ang)
        return [total[m * ns:(m + 1) * ns] for m in range(len(ns_of))]

    def spread_out(n, lines):
        a = origins_of[n]
        high, low = halves(lines)
        next_high, next_low = halves(pltpu.roll(lines, width - 1, 1))
        stack = jnp.concatenate([high, low, next_high, next_low], axis=0)
        for m in range(per_angle):
            z, part = m // per_row, m % per_row
            got = mm(stack, tables[n * per_angle + m])
            lower = got[:ns] + got[ns:2 * ns]
            upper = got[2 * ns:3 * ns] + got[3 * ns:]
            w = weight[pl.ds(a, 1), z, pl.ds(part * chunk, chunk)]
            value = (1.0 - w) * lower + w * upper
            lanes = pl.ds(m * chunk, chunk)
            recon[:, lanes] = value if n == 0 else recon[:, lanes] + value

    def whole_lines(ns_of):
        for n, lines in zip(ns_of, filtered(ns_of)):
            spread_out(n, lines)

    later = range(1, len(groups))
    for j in range(count):
        place_own(accr, whole_patch(j, 0), j)
    for n in range(n_ang - 1):
        pass_on(0, n)
        lay_own(0, n + 1)
    for g in range(len(groups)):
        lay_own(g, 0)
        lay_beside(g, 0)
    whole_lines([0])
    for g in later:
        for n in range(n_ang - 1):
            pass_on(g, n)
            if n == 0:
                share()
            lay_own(g, n + 1)
    if len(groups) == 1:
        share()
    for copy in second[-1][1]:
        copy.start()
    for g, group in enumerate(groups):
        for copy in second[g][0]:
            copy.wait()
        for j in group:
            place_above(acci, from_above[j, 1], j)
            place_below(acci, from_below[j, 1], j)
    for t in range(tiles):
        lanes = slice(t * LANES, (t + 1) * LANES)
        newobj[0, 1, :, lanes] = obj[1, t] + acci[t] * accw[t]
    for copy in early:
        copy.wait()
    for g in range(len(groups)):
        lay_beside(g, 1)
    whole_lines([1])
    for copy in gather:
        copy.wait()
    total = ag[0]
    for a in range(1, n_ang):
        total = total + ag[a]
    mine = pl.ds(pl.multiple_of(core * half + chip * pr, 8), pr)
    for c in range(2):
        value = total[c] / (total[2] + 1.0)
        piece[c] = value
        change[c, mine, :] = value
    spread = [
        remote(piece, change.at[:, mine, :], fin_send.at[d], fin_recv.at[d], "pos", peer)
        for d, peer in enumerate(pos_peers)
    ]
    for copy in spread:
        copy.start()
    for n in range(2, n_ang):
        for g in range(len(groups)):
            lay_beside(g, n)
    if n_ang > 2:
        whole_lines(list(range(2, n_ang)))
    for g, group in enumerate(groups):
        for copy in second[g][1]:
            copy.wait()
        for j in group:
            place_above(accr, from_above[j, 0], j)
            place_below(accr, from_below[j, 0], j)
    for t in range(tiles):
        lanes = slice(t * LANES, (t + 1) * LANES)
        newobj[0, 0, :, lanes] = obj[0, t] + accr[t] * accw[t]
    for copy in spread:
        copy.wait()


def tail_kernel(newobj, recon, change, probe, out_obj, out_probe, out_recon, sem):
    copy = pltpu.make_async_copy(newobj, out_obj, sem.at[0])
    copy.start()
    out_probe[...] = probe[...] + change[...]
    width = out_recon.shape[3]
    for s in range(out_recon.shape[1]):
        for z in range(out_recon.shape[2]):
            out_recon[0, s, z:z + 1, :] = recon[s:s + 1, z * width:(z + 1) * width]
    copy.wait()


def on_device(n_ang, n_pos, amplitude, offsets, probe_field, object_field, interp_index, interp_weight):
    band = object_field.shape[2]
    width = object_field.shape[3]
    patch = probe_field.shape[1]
    half = patch // 2
    count = offsets.shape[1]
    tiles = width // LANES
    f32, i32, bf16 = jnp.float32, jnp.int32, jnp.bfloat16
    n_z = interp_index.shape[1]
    chunk = min(512, width)
    tables = n_ang * n_z * (width // chunk)
    size = 2 if count % 2 == 0 else count
    left, right = dft_blocks(patch)
    ah, al = split_const(left)
    bh, bl = split_const(right)
    vmem = pl.BlockSpec(memory_space=VMEM)
    hbm = pl.BlockSpec(memory_space=pl.ANY)
    sds = jax.ShapeDtypeStruct
    dma = pltpu.SemaphoreType.DMA
    total = n_z * width
    ns = band // n_ang
    pr = patch // n_pos
    lead = max(0, band - half)
    ext = 2 * tiles
    table = VMEM((2 * patch, 2 * patch), bf16)
    half_shape = (count, 2, half, patch)
    bits = (n_ang - 1).bit_length()
    links = 2 + 6 * (count // size)
    base = [
        VMEM((2, tiles, band, LANES), f32), VMEM(amplitude.shape, f32), VMEM(probe_field.shape, f32),
        VMEM(interp_index.shape, i32), VMEM(interp_weight.shape, f32), table, table, table, table,
        [VMEM((size, 2, band + patch, patch), f32)] * (count // size), VMEM((2,) + half_shape, f32),
        VMEM((ext, lead + half + band, LANES), f32),
        VMEM((ext, half + band, LANES), f32), VMEM((ext, half + band, LANES), f32),
    ]
    sums = [
        VMEM((tiles, band, LANES), f32), VMEM((tiles, band, LANES), f32), VMEM((tiles, band, LANES), f32),
        VMEM((2,) + half_shape, f32), VMEM(half_shape, f32), VMEM(half_shape, f32),
    ]
    parts = [VMEM((3, patch, patch), f32), VMEM((n_pos - 1, 3, pr, patch), f32)]
    filters = [VMEM((tables, width, chunk), bf16), VMEM((width, width), bf16), VMEM((width, width), bf16)]
    groups, peers = count // size, n_ang - 1
    sems = [dma((9 + tiles,)), dma((links,)), dma((links,)), dma((n_pos - 1,)), dma((n_pos - 1,))]
    ends = [dma((n_pos - 1,)), dma((n_pos - 1,))]
    lines = VMEM((n_ang, tiles, ns, LANES), f32)
    offsets_of = pltpu.SMEM((2, count), i32)
    if band == patch:
        kernel = slice_kernel
        scratch = [
            offsets_of, pltpu.SMEM((2, 2, count), i32), pltpu.SMEM((peers, 2, count), i32),
            pltpu.SMEM((peers, 2, count), i32), *base, VMEM((ext, ns, LANES), f32), *sums,
            VMEM((size, 2 * patch, patch), f32), VMEM((count, band, patch), f32),
            VMEM((peers, tiles, ns, LANES), f32), VMEM((peers, count, ns, LANES), f32),
            VMEM((n_ang, count, ns, LANES), f32), lines, lines, *parts, VMEM((2, 3, half, patch), f32),
            VMEM((3, pr, patch), f32), VMEM((n_ang, 3, pr, patch), f32), VMEM((2, pr, patch), f32), *filters,
            *sems, dma((2,)), dma((peers,)), dma((peers,)), dma((peers,)), dma((peers,)), dma((peers,)), dma((peers,)),
            dma((peers, groups)), dma((peers, groups)), dma((n_ang, groups)), dma((n_ang, groups)),
            dma((peers,)), dma((peers,)), *ends,
        ]
    else:
        kernel = step_kernel
        scratch = [
            offsets_of, pltpu.SMEM((2, 2, count), i32), *base, *sums, *parts,
            VMEM((bits, 3, pr, patch), f32), VMEM((bits, 3, pr, patch), f32), VMEM((2, pr, patch), f32),
            VMEM((peers, ns, width), f32), *filters, *sems,
            dma((peers,)), dma((peers,)), dma((bits,)), dma((bits,)), *ends,
        ]
    newobj, recon, change = pl.pallas_call(
        functools.partial(kernel, n_ang, n_pos, size),
        out_shape=(VMEM(object_field.shape, f32), VMEM((ns, total), f32), VMEM(probe_field.shape, f32)),
        in_specs=[hbm] * 10,
        out_specs=(vmem,) * 3,
        scratch_shapes=scratch,
        compiler_params=pltpu.CompilerParams(
            collective_id=0, has_side_effects=True, vmem_limit_bytes=KLIMIT),
        name="step",
    )(*(pltpu.with_memory_space_constraint(x, pltpu.HBM) for x in (
        jnp.transpose(offsets[0]), object_field, amplitude, probe_field, interp_index, interp_weight,
        ah, al, bh, bl)))
    out = pl.pallas_call(
        tail_kernel,
        out_shape=(sds(object_field.shape, f32), sds(probe_field.shape, f32), sds((1, ns, n_z, width), f32)),
        in_specs=[vmem] * 4,
        out_specs=(hbm, vmem, vmem),
        scratch_shapes=[dma((1,))],
        compiler_params=pltpu.CompilerParams(vmem_limit_bytes=TLIMIT),
        name="tail",
    )(newobj, recon, change, probe_field)
    return tuple(out)


KLIMIT = 48 * 1024 * 1024
TLIMIT = 8 * 1024 * 1024


def solution(mesh):
    placed = (
        P("angle", "pos", None, None),
        P("angle", "pos", None),
        P(),
        P("angle", None, "pos", None),
        P(),
        P(),
    )
    return jax.shard_map(
        functools.partial(on_device, mesh.shape["angle"], mesh.shape["pos"]),
        mesh=mesh,
        in_specs=placed,
        out_specs=(P("angle", None, "pos", None), P(), P("pos", "angle", None, None)),
        check_vma=False,
    )
```

```python
import functools
import math

import jax
import jax.numpy as jnp
import numpy as np
from jax import lax
from jax.experimental import pallas as pl
from jax.experimental.pallas import tpu as pltpu
from jax.sharding import PartitionSpec as P

MESH = pl.DeviceIdType.MESH
VMEM = pltpu.VMEM
LANES = 128


def split_const(table):
    high = jnp.asarray(table, jnp.float32).astype(jnp.bfloat16)
    low = (jnp.asarray(table, jnp.float32) - high.astype(jnp.float32)).astype(jnp.bfloat16)
    return high, low


def dft_blocks(length):
    ramp = np.arange(length)
    theta = (ramp[:, None] * ramp[None, :] % length) * (2.0 * math.pi / length)
    real = np.cos(theta) / math.sqrt(length)
    imag = -np.sin(theta) / math.sqrt(length)
    left = np.block([[real, -imag], [imag, real]])
    right = np.block([[real, imag], [-imag, real]])
    return np.asarray(left, np.float32), np.asarray(right, np.float32)


def halves(value):
    high = value.astype(jnp.bfloat16)
    return high, (value - high.astype(jnp.float32)).astype(jnp.bfloat16)


def mm(a, b):
    return jnp.dot(a, b, preferred_element_type=jnp.float32)


def left3(table_high, table_low, value):
    high, low = halves(value)
    return mm(table_high, high) + mm(table_high, low) + mm(table_low, high)


def right3(value, table_high, table_low):
    high, low = halves(value)
    return mm(high, table_high) + mm(low, table_high) + mm(high, table_low)


def remote(src, dst, send, recv, axis, target):
    return pltpu.make_async_remote_copy(
        src_ref=src, dst_ref=dst, send_sem=send, recv_sem=recv,
        device_id={axis: target}, device_id_type=MESH,
    )


def flip(me, mask, bits):
    other = 0
    for b in range(bits):
        bit = (me // (1 << b)) % 2
        other = other + (1 << b) * (1 - bit if (mask >> b) & 1 else bit)
    return other


def step_kernel(n_ang, n_pos, size,
                offs_h, obj_h, amp_h, probe_h, index_h, weight_h, ah_h, al_h, bh_h, bl_h,
                newobj, recon, change,
                offs, near, obj, amp, probe, index, weight, ah, al, bh, bl,
                ext, sb, zo, za, zb, accw, acci, accr, grad, from_above, from_below,
                numden, rs, partial, ag, piece, sino, tables, rh, rl,
                in_sem, send_sem, recv_sem, rs_send, rs_recv,
                a2a_send, a2a_recv, ag_send, ag_recv, fin_send, fin_recv):
    me_a = lax.axis_index("angle")
    me = lax.axis_index("pos")
    up, down = lax.rem(me + n_pos - 1, n_pos), lax.rem(me + 1, n_pos)
    tiles, band = obj.shape[1], obj.shape[2]
    width = tiles * LANES
    patch = probe.shape[1]
    half = patch // 2
    count = amp.shape[1]
    ns = sino.shape[1]

    sources = [(offs_h, offs), (probe_h, probe), (amp_h, amp),
               (ah_h, ah), (al_h, al), (bh_h, bh), (bl_h, bl), (index_h, index), (weight_h, weight)]
    sources += [(obj_h.at[0, :, :, pl.ds(t * LANES, LANES)], obj.at[:, t]) for t in range(tiles)]
    loads = [pltpu.make_async_copy(src, dst, in_sem.at[k]) for k, (src, dst) in enumerate(sources)]
    for copy in loads:
        copy.start()
    bits = (n_ang - 1).bit_length()
    order = [1] + list(range(n_ang - 1, 1, -1))
    angle_peers = [flip(me_a, mask, bits) for mask in order]
    pos_peers = [lax.rem(me + d, n_pos) for d in range(1, n_pos)]
    barrier = pltpu.get_barrier_semaphore()
    for peer in pos_peers:
        pl.semaphore_signal(barrier, inc=1, device_id={"pos": peer}, device_id_type=MESH)
    for peer in angle_peers:
        pl.semaphore_signal(barrier, inc=1, device_id={"angle": peer}, device_id_type=MESH)
    loads[0].wait()
    pl.semaphore_wait(barrier, n_ang + n_pos - 2)
    swap = [remote(offs, near.at[0], send_sem.at[0], recv_sem.at[0], "pos", down),
            remote(offs, near.at[1], send_sem.at[1], recv_sem.at[1], "pos", up)]
    for copy in swap:
        copy.start()
    for copy in loads[9:]:
        copy.wait()

    def columns(c, rows, col):
        tile = col // LANES
        after = jnp.minimum(tile + 1, tiles - 1)
        got = jnp.concatenate([obj[c, tile, rows, :], obj[c, after, rows, :]], axis=1)
        return pltpu.roll(got, lax.rem(2 * LANES - lax.rem(col, LANES), 2 * LANES), 1)[:, :patch]

    for j in range(count):
        for c in range(2):
            ext[j // size][j % size, c, half:half + band, :] = columns(c, slice(0, band), offs[1, j])
    zo[...] = jnp.zeros_like(zo)
    za[...] = jnp.zeros_like(za)
    zb[...] = jnp.zeros_like(zb)
    for k, copy in enumerate(swap):
        copy.wait()
    first = []
    groups = [range(g * size, (g + 1) * size) for g in range(count // size)]
    for g, group in enumerate(groups):
        for j in group:
            for c in range(2):
                sb[0, j, c] = columns(c, slice(band - half, band), near[1, 1, j])
                sb[1, j, c] = columns(c, slice(0, half), near[0, 1, j])
        span = pl.ds(g * size, size)
        pair = [
            remote(sb.at[0, span], ext[g].at[:, :, pl.ds(0, half), :],
                   send_sem.at[2 + 6 * g], recv_sem.at[2 + 6 * g], "pos", down),
            remote(sb.at[1, span], ext[g].at[:, :, pl.ds(half + band, half), :],
                   send_sem.at[3 + 6 * g], recv_sem.at[3 + 6 * g], "pos", up),
        ]
        for copy in pair:
            copy.start()
        first.append(pair)

    def spot(row, col, owner):
        return jnp.clip(row - owner * band + half, 0, band), col

    own_at = [spot(offs[0, j], offs[1, j], me) for j in range(count)]
    above_at = [spot(near[0, 0, j], near[0, 1, j], up) for j in range(count)]
    below_at = [spot(near[1, 0, j], near[1, 1, j], down) for j in range(count)]

    def wide(plane, col):
        blank = jnp.zeros((plane.shape[0], LANES), jnp.float32)
        both = jnp.concatenate([plane, blank], axis=1)
        return pltpu.roll(both, lax.rem(col, LANES), 1)

    lead = max(0, band - half)

    def place(acc, buf, first_row, plane, start, rows, col):
        shifted = wide(plane, col)
        where = slice(first_row, first_row + plane.shape[0])
        buf[tiles - 1, where, :] = shifted[:, :LANES]
        buf[tiles, where, :] = shifted[:, LANES:]
        begin = tiles - 1 - col // LANES
        for t in range(tiles):
            acc[t, rows, :] = acc[t, rows, :] + buf[begin + t, pl.ds(start, rows.stop - rows.start), :]

    def place_own(acc, plane, j):
        row, col = own_at[j]
        place(acc, zo, lead, plane, lead + half - row, slice(0, band), col)

    def place_above(acc, plane, j):
        row, col = above_at[j]
        place(acc, za, 0, plane, band - row, slice(0, half), col)

    def place_below(acc, plane, j):
        row, col = below_at[j]
        place(acc, zb, band, plane, band - row, slice(band - half, band), col)

    loads[1].wait()
    p_re, p_im = probe[0], probe[1]
    power = p_re * p_re + p_im * p_im
    accw[...] = jnp.ones_like(accw)
    acci[...] = jnp.zeros_like(acci)
    accr[...] = jnp.zeros_like(accr)
    for j in range(count):
        place_own(accw, power, j)
        place_above(accw, power[half:], j)
        place_below(accw, power[:half], j)
    accw[...] = 1.0 / accw[...]
    tall = 64

    def ramp(step, carry):
        top = pl.multiple_of(step * tall, tall)
        shape = (tall, width)
        differ = lax.broadcasted_iota(jnp.int32, shape, 1) - (
            lax.broadcasted_iota(jnp.int32, shape, 0) + top)
        spread = differ.astype(jnp.float32)
        odd = -1.0 / (jnp.maximum(spread * spread, 1.0) * (math.pi * math.pi))
        value = jnp.where((differ & 1) == 1, odd, jnp.where(differ == 0, 0.25, 0.0))
        rh[pl.ds(top, tall), :], rl[pl.ds(top, tall), :] = halves(value)
        return carry

    lax.fori_loop(0, width // tall, ramp, 0)
    for copy in loads[2:9]:
        copy.wait()
    chunk = tables.shape[2]
    per_row = width // chunk
    zwin = index.shape[1]
    per_angle = zwin * per_row
    deep = 16
    pattern = lax.broadcasted_iota(jnp.int32, (deep, chunk), 0)
    one, zero = jnp.ones((deep, chunk), jnp.bfloat16), jnp.zeros((deep, chunk), jnp.bfloat16)
    pattern = pattern.astype(jnp.int16)

    origins = [me_a] + angle_peers

    def build(k, step, carry):
        a = origins[k]
        z = step // per_row
        lanes = pl.ds(pl.multiple_of(lax.rem(step, per_row) * chunk, chunk), chunk)
        at = jnp.broadcast_to(index[a, pl.ds(z, 1), lanes], (deep, chunk)).astype(jnp.int16)
        for r in range(width // deep):
            hit = at == pattern + jnp.int16(r * deep)
            tables[k * per_angle + step, r * deep:(r + 1) * deep, :] = jnp.where(hit, one, zero)
        return carry

    def build_all(k):
        lax.fori_loop(0, per_angle, functools.partial(build, k), 0)

    for k in range(n_ang):
        build_all(k)
    n_re = jnp.zeros((patch, patch), jnp.float32)
    n_im = n_re
    den = n_re
    second = []
    for g, group in enumerate(groups):
        for copy in first[g]:
            copy.wait()
        q_re, q_im, w_re, w_im = [], [], [], []
        for j in group:
            rows = pl.ds(own_at[j][0], patch)
            re, im = ext[g][j % size, 0, rows, :], ext[g][j % size, 1, rows, :]
            q_re.append(re)
            q_im.append(im)
            w_re.append(p_re * re - p_im * im)
            w_im.append(p_re * im + p_im * re)
        psi = jnp.concatenate([jnp.concatenate(w_re, axis=1), jnp.concatenate(w_im, axis=1)], axis=0)
        mid = left3(ah[...], al[...], psi)
        cells = [slice(n * patch, (n + 1) * patch) for n in range(size)]
        rows = [jnp.concatenate([mid[:patch, cell], mid[patch:, cell]], axis=1) for cell in cells]
        spec = right3(jnp.concatenate(rows, axis=0), bh[...], bl[...])
        fixed = []
        for j, cell in zip(group, cells):
            s_re = spec[cell, :patch]
            s_im = spec[cell, patch:]
            factor = amp[0, j] / jnp.maximum(jnp.sqrt(s_re * s_re + s_im * s_im), 0.5)
            fixed.append(jnp.concatenate([factor * s_re, factor * s_im], axis=1))
        back = right3(jnp.concatenate(fixed, axis=0), ah[...], al[...])
        wide_re = jnp.concatenate([back[cell, :patch] for cell in cells], axis=1)
        wide_im = jnp.concatenate([back[cell, patch:] for cell in cells], axis=1)
        diff = left3(bh[...], bl[...], jnp.concatenate([wide_re, wide_im], axis=0))
        diff = diff - psi
        for n, j in enumerate(group):
            d_re, d_im = diff[:patch, cells[n]], diff[patch:, cells[n]]
            g_re = p_re * d_re + p_im * d_im
            g_im = p_re * d_im - p_im * d_re
            for h in range(2):
                grad[h, j, 0] = g_re[h * half:(h + 1) * half]
                grad[h, j, 1] = g_im[h * half:(h + 1) * half]
            n_re = n_re + (q_re[n] * d_re + q_im[n] * d_im)
            n_im = n_im + (q_re[n] * d_im - q_im[n] * d_re)
            den = den + (q_re[n] * q_re[n] + q_im[n] * q_im[n])
        span = pl.ds(g * size, size)
        pairs = []
        for c in (1, 0):
            k = 4 + 6 * g + 2 * (1 - c)
            pairs.append([
                remote(grad.at[1, span, c], from_above.at[span, c], send_sem.at[k], recv_sem.at[k], "pos", down),
                remote(grad.at[0, span, c], from_below.at[span, c], send_sem.at[k + 1], recv_sem.at[k + 1], "pos", up),
            ])
        for copy in pairs[0] + ([] if g == len(groups) - 1 else pairs[1]):
            copy.start()
        second.append(pairs)
    numden[0] = n_re
    numden[1] = n_im
    numden[2] = den
    pr = patch // n_pos
    scatter = [
        remote(numden.at[:, pl.ds(pl.multiple_of(peer * pr, 8), pr), :], rs.at[d],
               rs_send.at[d], rs_recv.at[d], "pos", peer)
        for d, peer in enumerate(pos_peers)
    ]
    for copy in scatter + second[-1][1]:
        copy.start()

    def whole_patch(j, c):
        return jnp.concatenate([grad[0, j, c], grad[1, j, c]], axis=0)

    for j in range(count):
        place_own(acci, whole_patch(j, 1), j)
    for g, group in enumerate(groups):
        for copy in second[g][0]:
            copy.wait()
        for j in group:
            place_above(acci, from_above[j, 1], j)
            place_below(acci, from_below[j, 1], j)
    for t in range(tiles):
        lanes = slice(t * LANES, (t + 1) * LANES)
        newobj[0, 1, :, lanes] = obj[1, t] + acci[t] * accw[t]
    def project(k, a, lines):
        high, low = halves(lines)
        both = mm(jnp.concatenate([high, low], axis=0), rh[...])
        lines = (both[:ns] + both[ns:] + mm(high, rl[...])) * (math.pi / n_ang)
        high, low = halves(lines)
        next_high, next_low = halves(pltpu.roll(lines, width - 1, 1))
        stack = jnp.concatenate([high, low, next_high, next_low], axis=0)
        for n in range(per_angle):
            z, part = n // per_row, n % per_row
            got = mm(stack, tables[k * per_angle + n])
            lower = got[:ns] + got[ns:2 * ns]
            upper = got[2 * ns:3 * ns] + got[3 * ns:]
            w = weight[pl.ds(a, 1), z, pl.ds(part * chunk, chunk)]
            value = (1.0 - w) * lower + w * upper
            lanes = pl.ds(n * chunk, chunk)
            recon[:, lanes] = value if k == 0 else recon[:, lanes] + value

    across = [
        remote(newobj.at[0, 1, pl.ds(pl.multiple_of(peer * ns, 8), ns), :], sino.at[k],
               a2a_send.at[k], a2a_recv.at[k], "angle", peer)
        for k, peer in enumerate(angle_peers)
    ]
    inner = (me_a >= n_ang // 4) & (me_a < n_ang - n_ang // 4)
    across[0].start()

    @pl.when(inner)
    def _():
        for copy in across[1:-1]:
            copy.start()

    for copy in scatter:
        copy.wait()
    part = numden[:, pl.ds(pl.multiple_of(me * pr, 8), pr), :]
    for d in range(n_pos - 1):
        part = part + rs[d]
    partial[0] = part
    shares = [
        remote(partial.at[b], ag.at[b], ag_send.at[b], ag_recv.at[b], "angle", flip(me_a, 1 << b, bits))
        for b in range(bits)
    ]
    shares[0].start()

    @pl.when(jnp.logical_not(inner))
    def _():
        for copy in across[1:-1]:
            copy.start()

    project(0, me_a, newobj[0, 1, pl.ds(pl.multiple_of(me_a * ns, 8), ns), :])
    for b in range(bits - 1):
        shares[b].wait()
        partial[b + 1] = partial[b] + ag[b]
        shares[b + 1].start()
    across[-1].start()
    for g, group in enumerate(groups):
        for copy in second[g][1]:
            copy.wait()
        for j in group:
            place_own(accr, whole_patch(j, 0), j)
            place_above(accr, from_above[j, 0], j)
            place_below(accr, from_below[j, 0], j)
    for t in range(tiles):
        lanes = slice(t * LANES, (t + 1) * LANES)
        newobj[0, 0, :, lanes] = obj[0, t] + accr[t] * accw[t]
    shares[-1].wait()
    total = partial[bits - 1] + ag[bits - 1]
    mine = pl.ds(pl.multiple_of(me * pr, 8), pr)
    for c in range(2):
        value = total[c] / (total[2] + 1.0)
        piece[c] = value
        change[c, mine, :] = value
    spread = [
        remote(piece, change.at[:, mine, :], fin_send.at[d], fin_recv.at[d], "pos", peer)
        for d, peer in enumerate(pos_peers)
    ]
    for copy in spread:
        copy.start()
    for k, peer in enumerate(angle_peers):
        across[k].wait()
        project(k + 1, peer, sino[k])
    for copy in spread:
        copy.wait()


def slice_kernel(n_ang, n_pos, size,
                 offs_h, obj_h, amp_h, probe_h, index_h, weight_h, ah_h, al_h, bh_h, bl_h,
                 newobj, recon, change,
                 offs, near, far, farn, obj, amp, probe, index, weight, ah, al, bh, bl,
                 ext, sb, zo, za, zb, zq, accw, acci, accr, grad, from_above, from_below,
                 twice, blk, orx, rx, nrx, lw, lg,
                 numden, rs, paired, partial, ag, piece, tables, rh, rl,
                 in_sem, send_sem, recv_sem, rs_send, rs_recv, pair_sem, far_send, far_recv, farn_send, farn_recv,
                 o_send, o_recv, z_send, z_recv, f_send, f_recv, ag_send, ag_recv, fin_send, fin_recv):
    me_a = lax.axis_index("angle")
    me = lax.axis_index("pos")
    up, down = lax.rem(me + n_pos - 1, n_pos), lax.rem(me + 1, n_pos)
    tiles, band = obj.shape[1], obj.shape[2]
    width = tiles * LANES
    patch = probe.shape[1]
    half = patch // 2
    count = amp.shape[1]
    ns = orx.shape[2]
    side = (me_a * ns) // half
    ahead = lax.rem(me + n_pos + 1 - 2 * side, n_pos)
    behind = lax.rem(me + n_pos - 1 + 2 * side, n_pos)

    sources = [(offs_h, offs), (probe_h, probe), (amp_h, amp),
               (ah_h, ah), (al_h, al), (bh_h, bh), (bl_h, bl), (index_h, index), (weight_h, weight)]
    sources += [(obj_h.at[0, :, :, pl.ds(t * LANES, LANES)], obj.at[:, t]) for t in range(tiles)]
    loads = [pltpu.make_async_copy(src, dst, in_sem.at[k]) for k, (src, dst) in enumerate(sources)]
    bits = (n_ang - 1).bit_length()
    order = [1] + list(range(n_ang - 1, 1, -1))
    angle_peers = [flip(me_a, mask, bits) for mask in order]
    pos_peers = [lax.rem(me + d, n_pos) for d in range(1, n_pos)]
    barrier = pltpu.get_barrier_semaphore()
    for peer in pos_peers:
        pl.semaphore_signal(barrier, inc=1, device_id={"pos": peer}, device_id_type=MESH)
    for peer in angle_peers:
        pl.semaphore_signal(barrier, inc=1, device_id={"angle": peer}, device_id_type=MESH)
    for copy in loads:
        copy.start()
    loads[0].wait()
    pl.semaphore_wait(barrier, n_ang + n_pos - 2)
    swap = [remote(offs, near.at[0], send_sem.at[0], recv_sem.at[0], "pos", down),
            remote(offs, near.at[1], send_sem.at[1], recv_sem.at[1], "pos", up)]
    reach = [remote(offs, far.at[n], far_send.at[n], far_recv.at[n], "angle", peer)
             for n, peer in enumerate(angle_peers)]
    for copy in swap + reach:
        copy.start()
    for copy in loads[9:]:
        copy.wait()
    early = [remote(obj.at[1, :, pl.ds(pl.multiple_of(peer * ns, 8), ns), :], orx.at[n],
                    o_send.at[n], o_recv.at[n], "angle", peer)
             for n, peer in enumerate(angle_peers)]
    for copy in early:
        copy.start()

    def columns(c, rows, col):
        tile = col // LANES
        after = jnp.minimum(tile + 1, tiles - 1)
        got = jnp.concatenate([obj[c, tile, rows, :], obj[c, after, rows, :]], axis=1)
        return pltpu.roll(got, lax.rem(2 * LANES - lax.rem(col, LANES), 2 * LANES), 1)[:, :patch]

    for j in range(count):
        for c in range(2):
            ext[j // size][j % size, c, half:half + band, :] = columns(c, slice(0, band), offs[1, j])
    zo[...] = jnp.zeros_like(zo)
    za[...] = jnp.zeros_like(za)
    zb[...] = jnp.zeros_like(zb)
    zq[...] = jnp.zeros_like(zq)
    lg[...] = jnp.zeros_like(lg)
    lw[...] = jnp.ones_like(lw)
    for k, copy in enumerate(swap):
        copy.wait()
    relay = [remote(far.at[n], farn.at[n], farn_send.at[n], farn_recv.at[n], "pos", ahead)
             for n in range(n_ang - 1)]
    for n in range(n_ang - 1):
        reach[n].wait()
        relay[n].start()
    first = []
    groups = [range(g * size, (g + 1) * size) for g in range(count // size)]
    for g, group in enumerate(groups):
        for j in group:
            for c in range(2):
                sb[0, j, c] = columns(c, slice(band - half, band), near[1, 1, j])
                sb[1, j, c] = columns(c, slice(0, half), near[0, 1, j])
        span = pl.ds(g * size, size)
        pair = [
            remote(sb.at[0, span], ext[g].at[:, :, pl.ds(0, half), :],
                   send_sem.at[2 + 6 * g], recv_sem.at[2 + 6 * g], "pos", down),
            remote(sb.at[1, span], ext[g].at[:, :, pl.ds(half + band, half), :],
                   send_sem.at[3 + 6 * g], recv_sem.at[3 + 6 * g], "pos", up),
        ]
        for copy in pair:
            copy.start()
        first.append(pair)

    def spot(row, col, owner):
        return jnp.clip(row - owner * band + half, 0, band), col

    own_at = [spot(offs[0, j], offs[1, j], me) for j in range(count)]
    above_at = [spot(near[0, 0, j], near[0, 1, j], up) for j in range(count)]
    below_at = [spot(near[1, 0, j], near[1, 1, j], down) for j in range(count)]

    def wide(plane, col):
        blank = jnp.zeros((plane.shape[0], LANES), jnp.float32)
        both = jnp.concatenate([plane, blank], axis=1)
        return pltpu.roll(both, lax.rem(col, LANES), 1)

    lead = max(0, band - half)

    def place(acc, buf, first_row, plane, start, rows, col):
        shifted = wide(plane, col)
        where = slice(first_row, first_row + plane.shape[0])
        buf[tiles - 1, where, :] = shifted[:, :LANES]
        buf[tiles, where, :] = shifted[:, LANES:]
        begin = tiles - 1 - col // LANES
        for t in range(tiles):
            acc[t, rows, :] = acc[t, rows, :] + buf[begin + t, pl.ds(start, rows.stop - rows.start), :]

    def place_own(acc, plane, j):
        row, col = own_at[j]
        place(acc, zo, lead, plane, lead + half - row, slice(0, band), col)

    def place_above(acc, plane, j):
        row, col = above_at[j]
        place(acc, za, 0, plane, band - row, slice(0, half), col)

    def place_below(acc, plane, j):
        row, col = below_at[j]
        place(acc, zb, band, plane, band - row, slice(band - half, band), col)

    loads[1].wait()
    p_re, p_im = probe[0], probe[1]
    power = p_re * p_re + p_im * p_im
    accw[...] = jnp.ones_like(accw)
    acci[...] = jnp.zeros_like(acci)
    accr[...] = jnp.zeros_like(accr)
    for j in range(count):
        place_own(accw, power, j)
        place_above(accw, power[half:], j)
        place_below(accw, power[:half], j)
    accw[...] = 1.0 / accw[...]
    tall = 64

    def ramp(step, carry):
        top = pl.multiple_of(step * tall, tall)
        shape = (tall, width)
        differ = lax.broadcasted_iota(jnp.int32, shape, 1) - (
            lax.broadcasted_iota(jnp.int32, shape, 0) + top)
        spread = differ.astype(jnp.float32)
        odd = -1.0 / (jnp.maximum(spread * spread, 1.0) * (math.pi * math.pi))
        value = jnp.where((differ & 1) == 1, odd, jnp.where(differ == 0, 0.25, 0.0))
        rh[pl.ds(top, tall), :], rl[pl.ds(top, tall), :] = halves(value)
        return carry

    lax.fori_loop(0, width // tall, ramp, 0)
    for copy in loads[2:9]:
        copy.wait()
    chunk = tables.shape[2]
    per_row = width // chunk
    zwin = index.shape[1]
    per_angle = zwin * per_row
    deep = 16
    pattern = lax.broadcasted_iota(jnp.int32, (deep, chunk), 0)
    one, zero = jnp.ones((deep, chunk), jnp.bfloat16), jnp.zeros((deep, chunk), jnp.bfloat16)
    pattern = pattern.astype(jnp.int16)

    origins = [me_a] + angle_peers

    def build(k, step, carry):
        a = origins[k]
        z = step // per_row
        lanes = pl.ds(pl.multiple_of(lax.rem(step, per_row) * chunk, chunk), chunk)
        at = jnp.broadcast_to(index[a, pl.ds(z, 1), lanes], (deep, chunk)).astype(jnp.int16)
        for r in range(width // deep):
            hit = at == pattern + jnp.int16(r * deep)
            tables[k * per_angle + step, r * deep:(r + 1) * deep, :] = jnp.where(hit, one, zero)
        return carry

    def build_all(k):
        lax.fori_loop(0, per_angle, functools.partial(build, k), 0)

    for k in range(n_ang):
        build_all(k)
    places = [offs] + [far.at[n] for n in range(n_ang - 1)]
    behinds = [near.at[side]] + [farn.at[n] for n in range(n_ang - 1)]
    slot = lax.broadcasted_iota(jnp.int32, (ns, LANES), 0) + me_a * ns

    def mark(row, beside):
        if beside:
            return jnp.where(side == 0, (slot < row).astype(jnp.float32), (slot >= row + band).astype(jnp.float32))
        return ((slot >= row) & (slot < row + band)).astype(jnp.float32)

    def lay(acc, n, plane, col):
        shifted = wide(plane, col)
        zq[tiles - 1] = shifted[:, :LANES]
        zq[tiles] = shifted[:, LANES:]
        begin = tiles - 1 - col // LANES
        for t in range(tiles):
            acc[n, t] = acc[n, t] + zq[begin + t]

    def edge(n, j, beside):
        if beside:
            return behinds[n][0, j] - behind * band, behinds[n][1, j]
        return places[n][0, j] - me * band, places[n][1, j]

    for copy in relay:
        copy.wait()
    twice[0, :patch] = power
    twice[0, patch:] = power
    for n in range(n_ang):
        for beside in (False, True):
            for j in range(count):
                row, col = edge(n, j, beside)
                begin = lax.rem(me_a * ns + 2 * band - jnp.clip(row, -band, band), band)
                lay(lw, n, twice[0, pl.ds(begin, ns), :] * mark(row, beside), col)
    lw[...] = 1.0 / lw[...]

    n_re = jnp.zeros((patch, patch), jnp.float32)
    n_im = n_re
    den = n_re
    second, outward, forward = [], [], []
    for g, group in enumerate(groups):
        for copy in first[g]:
            copy.wait()
        q_re, q_im, w_re, w_im = [], [], [], []
        for j in group:
            rows = pl.ds(own_at[j][0], patch)
            re, im = ext[g][j % size, 0, rows, :], ext[g][j % size, 1, rows, :]
            q_re.append(re)
            q_im.append(im)
            w_re.append(p_re * re - p_im * im)
            w_im.append(p_re * im + p_im * re)
        psi = jnp.concatenate([jnp.concatenate(w_re, axis=1), jnp.concatenate(w_im, axis=1)], axis=0)
        mid = left3(ah[...], al[...], psi)
        cells = [slice(n * patch, (n + 1) * patch) for n in range(size)]
        rows = [jnp.concatenate([mid[:patch, cell], mid[patch:, cell]], axis=1) for cell in cells]
        spec = right3(jnp.concatenate(rows, axis=0), bh[...], bl[...])
        fixed = []
        for j, cell in zip(group, cells):
            s_re = spec[cell, :patch]
            s_im = spec[cell, patch:]
            factor = amp[0, j] / jnp.maximum(jnp.sqrt(s_re * s_re + s_im * s_im), 0.5)
            fixed.append(jnp.concatenate([factor * s_re, factor * s_im], axis=1))
        back = right3(jnp.concatenate(fixed, axis=0), ah[...], al[...])
        wide_re = jnp.concatenate([back[cell, :patch] for cell in cells], axis=1)
        wide_im = jnp.concatenate([back[cell, patch:] for cell in cells], axis=1)
        diff = left3(bh[...], bl[...], jnp.concatenate([wide_re, wide_im], axis=0))
        diff = diff - psi
        for n, j in enumerate(group):
            d_re, d_im = diff[:patch, cells[n]], diff[patch:, cells[n]]
            g_re = p_re * d_re + p_im * d_im
            g_im = p_re * d_im - p_im * d_re
            twice[n, :patch] = g_im
            twice[n, patch:] = g_im
            blk[j] = twice[n, pl.ds(lax.rem(2 * band - (offs[0, j] - me * band), band), band), :]
            for h in range(2):
                grad[h, j, 0] = g_re[h * half:(h + 1) * half]
                grad[h, j, 1] = g_im[h * half:(h + 1) * half]
            n_re = n_re + (q_re[n] * d_re + q_im[n] * d_im)
            n_im = n_im + (q_re[n] * d_im - q_im[n] * d_re)
            den = den + (q_re[n] * q_re[n] + q_im[n] * q_im[n])
        span = pl.ds(g * size, size)
        out = [remote(blk.at[span, pl.ds(pl.multiple_of(peer * ns, 8), ns), :], rx.at[n, span],
                      z_send.at[n, g], z_recv.at[n, g], "angle", peer)
               for n, peer in enumerate(angle_peers)]
        mine = remote(blk.at[span, pl.ds(pl.multiple_of(me_a * ns, 8), ns), :], nrx.at[0, span],
                      f_send.at[0, g], f_recv.at[0, g], "pos", ahead)
        for copy in out + [mine]:
            copy.start()
        outward.append(out)
        forward.append([mine])
        pairs = []
        for c in (1, 0):
            k = 4 + 6 * g + 2 * (1 - c)
            pairs.append([
                remote(grad.at[1, span, c], from_above.at[span, c], send_sem.at[k], recv_sem.at[k], "pos", down),
                remote(grad.at[0, span, c], from_below.at[span, c], send_sem.at[k + 1], recv_sem.at[k + 1], "pos", up),
            ])
        for copy in pairs[0] + ([] if g == len(groups) - 1 else pairs[1]):
            copy.start()
        second.append(pairs)
    numden[0] = n_re
    numden[1] = n_im
    numden[2] = den
    pr = patch // n_pos
    core, chip, chips = me % 2, me // 2, n_pos // 2
    swap_half = remote(numden.at[:, pl.ds(pl.multiple_of((1 - core) * half, 8), half), :], paired.at[0],
                       pair_sem.at[0], pair_sem.at[1], "pos", me + 1 - 2 * core)
    swap_half.start()

    def whole_patch(j, c):
        return jnp.concatenate([grad[0, j, c], grad[1, j, c]], axis=0)

    for j in range(count):
        place_own(acci, whole_patch(j, 1), j)
    swap_half.wait()
    paired[1] = paired[0] + numden[:, pl.ds(pl.multiple_of(core * half, 8), half), :]
    chip_peers = [lax.rem(chip + d, chips) for d in range(1, chips)]
    scatter = [
        remote(paired.at[1, :, pl.ds(pl.multiple_of(peer * pr, 8), pr), :], rs.at[d],
               rs_send.at[d], rs_recv.at[d], "pos", 2 * peer + core)
        for d, peer in enumerate(chip_peers)
    ]
    for copy in scatter:
        copy.start()

    def pass_on(g, n):
        outward[g][n].wait()
        copy = remote(rx.at[n, pl.ds(g * size, size)], nrx.at[n + 1, pl.ds(g * size, size)],
                      f_send.at[n + 1, g], f_recv.at[n + 1, g], "pos", ahead)
        copy.start()
        forward[g].append(copy)

    gather = [remote(partial, ag.at[me_a], ag_send.at[n], ag_recv.at[n], "angle", peer)
              for n, peer in enumerate(angle_peers)]

    def share():
        for copy in scatter:
            copy.wait()
        part = paired[1, :, pl.ds(pl.multiple_of(chip * pr, 8), pr), :]
        for d in range(chips - 1):
            part = part + rs[d]
        partial[...] = part
        ag[me_a] = part
        for copy in gather:
            copy.start()

    origins_of = [me_a] + angle_peers
    here = pl.ds(pl.multiple_of(me_a * ns, 8), ns)

    def lay_own(g, n):
        for j in groups[g]:
            row, col = edge(n, j, False)
            own = blk[j, here, :] if n == 0 else rx[n - 1, j]
            lay(lg, n, own * mark(row, False), col)

    def lay_beside(g, n):
        forward[g][n].wait()
        for j in groups[g]:
            row, col = edge(n, j, True)
            lay(lg, n, nrx[n, j] * mark(row, True), col)

    def filtered(ns_of):
        tops, lows = [], []
        for n in ns_of:
            parts = []
            for t in range(tiles):
                base = obj[1, t, here, :] if n == 0 else orx[n - 1, t]
                parts.append(base + lg[n, t] * lw[n, t])
            high, low = halves(jnp.concatenate(parts, axis=1))
            tops.append(high)
            lows.append(low)
        both = mm(jnp.concatenate(tops + lows, axis=0), rh[...])
        more = mm(jnp.concatenate(tops, axis=0), rl[...])
        size_of = len(ns_of) * ns
        total = (both[:size_of] + both[size_of:] + more) * (math.pi / n_ang)
        return [total[m * ns:(m + 1) * ns] for m in range(len(ns_of))]

    def spread_out(n, lines):
        a = origins_of[n]
        high, low = halves(lines)
        next_high, next_low = halves(pltpu.roll(lines, width - 1, 1))
        stack = jnp.concatenate([high, low, next_high, next_low], axis=0)
        for m in range(per_angle):
            z, part = m // per_row, m % per_row
            got = mm(stack, tables[n * per_angle + m])
            lower = got[:ns] + got[ns:2 * ns]
            upper = got[2 * ns:3 * ns] + got[3 * ns:]
            w = weight[pl.ds(a, 1), z, pl.ds(part * chunk, chunk)]
            value = (1.0 - w) * lower + w * upper
            lanes = pl.ds(m * chunk, chunk)
            recon[:, lanes] = value if n == 0 else recon[:, lanes] + value

    def whole_lines(ns_of):
        for n, lines in zip(ns_of, filtered(ns_of)):
            spread_out(n, lines)

    later = range(1, len(groups))
    for j in range(count):
        place_own(accr, whole_patch(j, 0), j)
    for n in range(n_ang - 1):
        pass_on(0, n)
        lay_own(0, n + 1)
    for g in range(len(groups)):
        lay_own(g, 0)
        lay_beside(g, 0)
    whole_lines([0])
    share()
    for g in later:
        for n in range(n_ang - 1):
            pass_on(g, n)
            lay_own(g, n + 1)
    for copy in second[-1][1]:
        copy.start()
    for g, group in enumerate(groups):
        for copy in second[g][0]:
            copy.wait()
        for j in group:
            place_above(acci, from_above[j, 1], j)
            place_below(acci, from_below[j, 1], j)
    for t in range(tiles):
        lanes = slice(t * LANES, (t + 1) * LANES)
        newobj[0, 1, :, lanes] = obj[1, t] + acci[t] * accw[t]
    for copy in early:
        copy.wait()
    for g in range(len(groups)):
        lay_beside(g, 1)
    whole_lines([1])
    for copy in gather:
        copy.wait()
    total = ag[0]
    for a in range(1, n_ang):
        total = total + ag[a]
    mine = pl.ds(pl.multiple_of(core * half + chip * pr, 8), pr)
    for c in range(2):
        value = total[c] / (total[2] + 1.0)
        piece[c] = value
        change[c, mine, :] = value
    spread = [
        remote(piece, change.at[:, mine, :], fin_send.at[d], fin_recv.at[d], "pos", peer)
        for d, peer in enumerate(pos_peers)
    ]
    for copy in spread:
        copy.start()
    for n in range(2, n_ang):
        for g in range(len(groups)):
            lay_beside(g, n)
    if n_ang > 2:
        whole_lines(list(range(2, n_ang)))
    for g, group in enumerate(groups):
        for copy in second[g][1]:
            copy.wait()
        for j in group:
            place_above(accr, from_above[j, 0], j)
            place_below(accr, from_below[j, 0], j)
    for t in range(tiles):
        lanes = slice(t * LANES, (t + 1) * LANES)
        newobj[0, 0, :, lanes] = obj[0, t] + accr[t] * accw[t]
    for copy in spread:
        copy.wait()


def tail_kernel(newobj, recon, change, probe, out_obj, out_probe, out_recon, sem):
    copy = pltpu.make_async_copy(newobj, out_obj, sem.at[0])
    copy.start()
    out_probe[...] = probe[...] + change[...]
    width = out_recon.shape[3]
    for s in range(out_recon.shape[1]):
        for z in range(out_recon.shape[2]):
            out_recon[0, s, z:z + 1, :] = recon[s:s + 1, z * width:(z + 1) * width]
    copy.wait()


def on_device(n_ang, n_pos, amplitude, offsets, probe_field, object_field, interp_index, interp_weight):
    band = object_field.shape[2]
    width = object_field.shape[3]
    patch = probe_field.shape[1]
    half = patch // 2
    count = offsets.shape[1]
    tiles = width // LANES
    f32, i32, bf16 = jnp.float32, jnp.int32, jnp.bfloat16
    n_z = interp_index.shape[1]
    chunk = min(512, width)
    tables = n_ang * n_z * (width // chunk)
    size = 2 if count % 2 == 0 else count
    left, right = dft_blocks(patch)
    ah, al = split_const(left)
    bh, bl = split_const(right)
    vmem = pl.BlockSpec(memory_space=VMEM)
    hbm = pl.BlockSpec(memory_space=pl.ANY)
    sds = jax.ShapeDtypeStruct
    dma = pltpu.SemaphoreType.DMA
    total = n_z * width
    ns = band // n_ang
    pr = patch // n_pos
    lead = max(0, band - half)
    ext = 2 * tiles
    table = VMEM((2 * patch, 2 * patch), bf16)
    half_shape = (count, 2, half, patch)
    bits = (n_ang - 1).bit_length()
    links = 2 + 6 * (count // size)
    base = [
        VMEM((2, tiles, band, LANES), f32), VMEM(amplitude.shape, f32), VMEM(probe_field.shape, f32),
        VMEM(interp_index.shape, i32), VMEM(interp_weight.shape, f32), table, table, table, table,
        [VMEM((size, 2, band + patch, patch), f32)] * (count // size), VMEM((2,) + half_shape, f32),
        VMEM((ext, lead + half + band, LANES), f32),
        VMEM((ext, half + band, LANES), f32), VMEM((ext, half + band, LANES), f32),
    ]
    sums = [
        VMEM((tiles, band, LANES), f32), VMEM((tiles, band, LANES), f32), VMEM((tiles, band, LANES), f32),
        VMEM((2,) + half_shape, f32), VMEM(half_shape, f32), VMEM(half_shape, f32),
    ]
    parts = [VMEM((3, patch, patch), f32), VMEM((n_pos - 1, 3, pr, patch), f32)]
    filters = [VMEM((tables, width, chunk), bf16), VMEM((width, width), bf16), VMEM((width, width), bf16)]
    groups, peers = count // size, n_ang - 1
    sems = [dma((9 + tiles,)), dma((links,)), dma((links,)), dma((n_pos - 1,)), dma((n_pos - 1,))]
    ends = [dma((n_pos - 1,)), dma((n_pos - 1,))]
    lines = VMEM((n_ang, tiles, ns, LANES), f32)
    offsets_of = pltpu.SMEM((2, count), i32)
    if band == patch:
        kernel = slice_kernel
        scratch = [
            offsets_of, pltpu.SMEM((2, 2, count), i32), pltpu.SMEM((peers, 2, count), i32),
            pltpu.SMEM((peers, 2, count), i32), *base, VMEM((ext, ns, LANES), f32), *sums,
            VMEM((size, 2 * patch, patch), f32), VMEM((count, band, patch), f32),
            VMEM((peers, tiles, ns, LANES), f32), VMEM((peers, count, ns, LANES), f32),
            VMEM((n_ang, count, ns, LANES), f32), lines, lines, *parts, VMEM((2, 3, half, patch), f32),
            VMEM((3, pr, patch), f32), VMEM((n_ang, 3, pr, patch), f32), VMEM((2, pr, patch), f32), *filters,
            *sems, dma((2,)), dma((peers,)), dma((peers,)), dma((peers,)), dma((peers,)), dma((peers,)), dma((peers,)),
            dma((peers, groups)), dma((peers, groups)), dma((n_ang, groups)), dma((n_ang, groups)),
            dma((peers,)), dma((peers,)), *ends,
        ]
    else:
        kernel = step_kernel
        scratch = [
            offsets_of, pltpu.SMEM((2, 2, count), i32), *base, *sums, *parts,
            VMEM((bits, 3, pr, patch), f32), VMEM((bits, 3, pr, patch), f32), VMEM((2, pr, patch), f32),
            VMEM((peers, ns, width), f32), *filters, *sems,
            dma((peers,)), dma((peers,)), dma((bits,)), dma((bits,)), *ends,
        ]
    newobj, recon, change = pl.pallas_call(
        functools.partial(kernel, n_ang, n_pos, size),
        out_shape=(VMEM(object_field.shape, f32), VMEM((ns, total), f32), VMEM(probe_field.shape, f32)),
        in_specs=[hbm] * 10,
        out_specs=(vmem,) * 3,
        scratch_shapes=scratch,
        compiler_params=pltpu.CompilerParams(
            collective_id=0, has_side_effects=True, vmem_limit_bytes=KLIMIT),
        name="step",
    )(*(pltpu.with_memory_space_constraint(x, pltpu.HBM) for x in (
        jnp.transpose(offsets[0]), object_field, amplitude, probe_field, interp_index, interp_weight,
        ah, al, bh, bl)))
    out = pl.pallas_call(
        tail_kernel,
        out_shape=(sds(object_field.shape, f32), sds(probe_field.shape, f32), sds((1, ns, n_z, width), f32)),
        in_specs=[vmem] * 4,
        out_specs=(hbm, vmem, vmem),
        scratch_shapes=[dma((1,))],
        compiler_params=pltpu.CompilerParams(vmem_limit_bytes=TLIMIT),
        name="tail",
    )(newobj, recon, change, probe_field)
    return tuple(out)


KLIMIT = 48 * 1024 * 1024
TLIMIT = 8 * 1024 * 1024


def solution(mesh):
    placed = (
        P("angle", "pos", None, None),
        P("angle", "pos", None),
        P(),
        P("angle", None, "pos", None),
        P(),
        P(),
    )
    return jax.shard_map(
        functools.partial(on_device, mesh.shape["angle"], mesh.shape["pos"]),
        mesh=mesh,
        in_specs=placed,
        out_specs=(P("angle", None, "pos", None), P(), P("pos", "angle", None, None)),
        check_vma=False,
    )
```
